32 devices in a mesh: dp: 1 (over z), ep_b: 4 (over y), ep_a: 8 (over x, core).
Axes of the slice: x: 4, y: 4, z: 1, core: 2. Of those that a mesh axis runs over, the one named last changes fastest.
The devices are a block of a 4x4x8 slice.
Arguments:
- tokens: bfloat16 [32, 8192, 384], P(('dp', 'ep_b', 'ep_a'))
- expert_ids: int32 [32, 8192], P(('dp', 'ep_b', 'ep_a'))
- route_order: int32 [32, 8192], P(('dp', 'ep_b', 'ep_a'))
- w_route: bfloat16 [384, 256], replicated
- expert_keys: bfloat16 [32, 256], replicated
- temperature: float32 [], replicated
- w_in: bfloat16 [32, 384, 1536], P(('ep_b', 'ep_a'))
- b_in: bfloat16 [32, 1536], P(('ep_b', 'ep_a'))
- w_out: bfloat16 [32, 1536, 384], P(('ep_b', 'ep_a'))
- b_out: bfloat16 [32, 384], P(('ep_b', 'ep_a'))
Outputs:
- output: bfloat16 [32, 8192, 384], P(('dp', 'ep_b', 'ep_a'))
All inputs are finite; a program needn't handle non-finite values.
Results may differ from the reference program's by a relative error of at most 0.00500943.
Values are sent between devices in bfloat16 or wider.
A program may use at most 768 MiB of HBM per device.

```python
import jax
import jax.numpy as jnp
from jax import lax

TOKENS_DEV = 8192
MODEL_DIM = 384
HIDDEN_DIM = 1536
ROUTER_DIM = 256
NUM_EXPERTS = 32
CAPACITY = 320
HOT_SPAN = max(1, NUM_EXPERTS // 4)


def draw_routes(route_key):
    key_list = jax.random.split(route_key, 5)
    shape_ids = (NUM_EXPERTS, TOKENS_DEV)
    spread_ids = jax.random.randint(key_list[0], shape_ids, 0, NUM_EXPERTS)
    hot_pick = jax.random.randint(key_list[1], shape_ids, 0, 4) == 0
    hot_base = jax.random.randint(key_list[2], (NUM_EXPERTS, 1), 0, NUM_EXPERTS)
    hot_ids = (hot_base + jax.random.randint(key_list[3], shape_ids, 0, HOT_SPAN)) % NUM_EXPERTS
    expert_ids = jnp.where(hot_pick, hot_ids, spread_ids).astype(jnp.int32)
    order_keys = jax.random.split(key_list[4], NUM_EXPERTS)
    route_order = jax.vmap(lambda order_key: jax.random.permutation(order_key, TOKENS_DEV))(order_keys)
    return expert_ids, route_order.astype(jnp.int32)


def setup_inputs(seed: int = 0, part: int = 0) -> dict:
    shared_keys = jax.random.split(jax.random.key(seed), 7)
    part_keys = jax.random.split(jax.random.fold_in(jax.random.key(seed + 1), part), 3)
    w_route = jax.random.normal(shared_keys[0], (MODEL_DIM, ROUTER_DIM), jnp.float32) * MODEL_DIM ** -0.5
    expert_keys = jax.random.normal(shared_keys[1], (NUM_EXPERTS, ROUTER_DIM), jnp.float32)
    temperature = jax.random.uniform(shared_keys[2], (), jnp.float32, 0.1, 0.16)
    w_in = jax.random.normal(shared_keys[3], (NUM_EXPERTS, MODEL_DIM, HIDDEN_DIM), jnp.float32) * MODEL_DIM ** -0.5
    b_in = jax.random.normal(shared_keys[4], (NUM_EXPERTS, HIDDEN_DIM), jnp.float32) * 0.5
    w_out = jax.random.normal(shared_keys[5], (NUM_EXPERTS, HIDDEN_DIM, MODEL_DIM), jnp.float32) * HIDDEN_DIM ** -0.5
    b_out = jax.random.normal(shared_keys[6], (NUM_EXPERTS, MODEL_DIM), jnp.float32) * 0.5
    expert_ids, route_order = draw_routes(part_keys[0])
    key_proj = jnp.dot(expert_keys, w_route.T)
    noise_rows = jax.random.normal(part_keys[1], (NUM_EXPERTS, TOKENS_DEV, MODEL_DIM), jnp.float32)
    strength = jax.random.uniform(part_keys[2], (NUM_EXPERTS, TOKENS_DEV, 1), jnp.float32, 0.5, 1.5)
    tokens = noise_rows + strength * key_proj[expert_ids]
    return {
        "tokens": tokens.astype(jnp.bfloat16),
        "expert_ids": expert_ids,
        "route_order": route_order,
        "w_route": w_route.astype(jnp.bfloat16),
        "expert_keys": expert_keys.astype(jnp.bfloat16),
        "temperature": temperature,
        "w_in": w_in.astype(jnp.bfloat16),
        "b_in": b_in.astype(jnp.bfloat16),
        "w_out": w_out.astype(jnp.bfloat16),
        "b_out": b_out.astype(jnp.bfloat16),
    }


def device_route(tok_rows, id_row, order_row, w_route, key_unit, temperature):
    projected = jnp.dot(tok_rows, w_route, preferred_element_type=jnp.float32)
    proj_unit = projected / jnp.sqrt(jnp.sum(projected * projected, axis=1, keepdims=True))
    router_prob = jax.nn.softmax(jnp.dot(proj_unit, key_unit.T) / temperature, axis=1)
    gate_prob = jnp.take_along_axis(router_prob, id_row[:, None], axis=1)[:, 0]
    ranked_ids = id_row[order_row]
    ranked_hot = (ranked_ids[:, None] == jnp.arange(NUM_EXPERTS)[None, :]).astype(jnp.int32)
    ranked_pos = jnp.sum(jnp.cumsum(ranked_hot, axis=0) * ranked_hot, axis=1) - 1
    slot_pos = jnp.zeros((TOKENS_DEV,), jnp.int32).at[order_row].set(ranked_pos)
    dest_slot = jnp.where(slot_pos < CAPACITY, id_row * CAPACITY + slot_pos, NUM_EXPERTS * CAPACITY)
    send_rows = jnp.zeros((NUM_EXPERTS * CAPACITY, MODEL_DIM), jnp.bfloat16).at[dest_slot].set(tok_rows, mode="drop")
    return send_rows, gate_prob, dest_slot


def expert_apply(operands):
    slot_rows, w_first, b_first, w_second, b_second = operands
    hidden = jnp.dot(slot_rows, w_first, preferred_element_type=jnp.float32) + b_first.astype(jnp.float32)
    hidden = jax.nn.gelu(hidden, approximate=False).astype(jnp.bfloat16)
    result = jnp.dot(hidden, w_second, preferred_element_type=jnp.float32) + b_second.astype(jnp.float32)
    return result.astype(jnp.bfloat16)


def reference(tokens, expert_ids, route_order, w_route, expert_keys, temperature, w_in, b_in, w_out, b_out):
    keys_f32 = expert_keys.astype(jnp.float32)
    key_unit = keys_f32 / jnp.sqrt(jnp.sum(keys_f32 * keys_f32, axis=1, keepdims=True))

    def route_one(operands):
        tok_rows, id_row, order_row = operands
        return device_route(tok_rows, id_row, order_row, w_route, key_unit, temperature)

    send_rows, gate_prob, dest_slot = lax.map(route_one, (tokens, expert_ids, route_order))
    grid_rows = send_rows.reshape(NUM_EXPERTS, NUM_EXPERTS, CAPACITY, MODEL_DIM)
    arrived = jnp.swapaxes(grid_rows, 0, 1).reshape(NUM_EXPERTS, NUM_EXPERTS * CAPACITY, MODEL_DIM)
    expert_out = lax.map(expert_apply, (arrived, w_in, b_in, w_out, b_out))
    returned = jnp.swapaxes(expert_out.reshape(NUM_EXPERTS, NUM_EXPERTS, CAPACITY, MODEL_DIM), 0, 1)
    returned = returned.reshape(NUM_EXPERTS, NUM_EXPERTS * CAPACITY, MODEL_DIM)

    def combine_one(operands):
        back_rows, dest_row, gate_row = operands
        picked = jnp.take(back_rows, dest_row, axis=0, mode="fill", fill_value=0)
        return (gate_row[:, None] * picked.astype(jnp.float32)).astype(jnp.bfloat16)

    return lax.map(combine_one, (returned, dest_slot, gate_prob))
```

```python
import functools

import jax
import jax.numpy as jnp
from jax import lax
from jax.experimental import pallas as pl
from jax.experimental.pallas import tpu as pltpu
from jax.sharding import PartitionSpec as P

EXPERT_AXES = ("ep_b", "ep_a")
LANES = 128
MESH_ID = pl.DeviceIdType.MESH
F32 = jnp.float32
BF16 = jnp.bfloat16


def iota(shape, dim):
    return lax.broadcasted_iota(jnp.int32, shape, dim)


def dot_nt(a, b):
    return lax.dot_general(a, b, (((1,), (1,)), ((), ())), preferred_element_type=F32)


def as_bf16(mask):
    return jnp.where(mask, 1.0, 0.0).astype(BF16)


def virtual_expert(ids, size_b, size_x):
    i_b, i_a = ids // (2 * size_x), ids % (2 * size_x)
    x, core = i_a // 2, i_a % 2
    return jnp.where(core == 0, x * size_b + i_b, size_b * size_x + i_b * size_x + x)


def dispatch_kernel(dims, ids_ref, order_ref, tok_hbm, send_hbm, dest_ref,
                    tok_vm, big, src_vm, src_sm, tmp, out_vm, tok_sem, src_sem, out_sem):
    size_b, size_x, cap = dims
    rows = ids_ref.shape[0]
    num_experts = 2 * size_b * size_x
    width = tok_vm.shape[1]
    parts = width // LANES
    slot_rows = src_vm.shape[0]
    tok_copy = pltpu.make_async_copy(tok_hbm, tok_vm, tok_sem)
    tok_copy.start()

    upper = as_bf16((iota((LANES, 2 * LANES), 0) <= iota((LANES, 2 * LANES), 1)) | (iota((LANES, 2 * LANES), 1) >= LANES))
    ids_t = ids_ref[...].astype(F32).T.astype(BF16)
    iota_rows = iota((rows, LANES), 0)
    iota_lane = iota((LANES, LANES), 0)
    iota_exp = iota((num_experts, LANES), 0)

    def ranked(r, carry):
        count, keep = carry
        o = order_ref[pl.ds(r, 1), :]
        hi, lo = o // LANES, o % LANES
        pick_hi = iota_rows == hi
        pick_lo = iota_lane == lo
        table = jnp.dot(ids_t, as_bf16(pick_hi), preferred_element_type=F32)
        rid = jnp.sum(jnp.where(pick_lo, table, 0.0), axis=0, keepdims=True)
        mine = iota_exp.astype(F32) == rid
        both = jnp.dot(as_bf16(mine), upper, preferred_element_type=F32)
        rank = jnp.sum(jnp.where(mine, both[:, :LANES] + count, 0.0), axis=0, keepdims=True)
        kept = rank <= float(cap)
        keep = keep + dot_nt(as_bf16(pick_hi & kept), as_bf16(pick_lo))
        return count + both[:, LANES:], keep

    zero_count = jnp.zeros((num_experts, LANES), F32)
    _, keep = lax.fori_loop(0, rows, ranked, (zero_count, jnp.zeros((rows, LANES), F32)), unroll=8)
    dest_ref[...] = keep.astype(jnp.int32)

    iota_slot = iota((slot_rows, LANES), 0)
    lane = iota((1, LANES), 1).astype(F32)

    def placed(r, carry):
        count, source = carry
        expert = virtual_expert(ids_ref[pl.ds(r, 1), :], size_b, size_x)
        kept = dest_ref[pl.ds(r, 1), :] > 0
        mine = (iota_exp == expert) & kept
        both = jnp.dot(as_bf16(mine), upper, preferred_element_type=F32)
        pos = jnp.sum(jnp.where(mine, both[:, :LANES] + count, 0.0), axis=0, keepdims=True) - 1.0
        slot = jnp.where(kept, expert * cap + pos.astype(jnp.int32), num_experts * cap)
        dest_ref[pl.ds(r, 1), :] = slot * parts
        pick = jnp.where(iota_slot == slot // LANES, 1.0, 0.0)
        stacked = jnp.concatenate([pick * lax.convert_element_type(r, F32), pick * lane], axis=0).astype(BF16)
        source = source + dot_nt(stacked, as_bf16(iota_lane == slot % LANES))
        return count + both[:, LANES:], source

    _, source = lax.fori_loop(0, rows, placed, (zero_count, jnp.zeros((2 * slot_rows, LANES), F32)), unroll=4)
    src_vm[...] = ((source[:slot_rows] * float(LANES) + source[slot_rows:]) * float(parts)).astype(jnp.int32)
    src_copy = pltpu.make_async_copy(src_vm, src_sm, src_sem)
    src_copy.start()

    tok_copy.wait()

    def widen(i, _):
        base = pl.multiple_of(i * 16, 16)
        for c in range(parts):
            big[pl.ds(base * parts + c, 16, stride=parts), :] = tok_vm[pl.ds(base, 16), c * LANES:(c + 1) * LANES].astype(F32)
        return 0

    lax.fori_loop(0, tok_vm.shape[0] // 16, widen, 0, unroll=8)
    src_copy.wait()

    def out_copy(i):
        return pltpu.make_async_copy(out_vm.at[lax.rem(i, 4)], send_hbm.at[pl.ds(pl.multiple_of(i * LANES, LANES), LANES)],
                                     out_sem.at[lax.rem(i, 4)])

    def gather(i, _):
        @pl.when(i >= 4)
        def _():
            out_copy(i - 4).wait()
        slot = lax.rem(i, 4)
        for j in range(LANES):
            tmp[pl.ds(j * parts, parts), :] = big[pl.ds(src_sm[i, j], parts), :]
        for j in range(0, LANES, 16):
            for c in range(parts):
                out_vm[slot, pl.ds(j, 16), c * LANES:(c + 1) * LANES] = tmp[pl.ds(j * parts + c, 16, stride=parts), :].astype(BF16)
        out_copy(i).start()
        return 0

    lax.fori_loop(0, slot_rows, gather, 0)
    for i in range(slot_rows - 4, slot_rows):
        out_copy(i).wait()


def dispatch(tok_rows, ids, order, dims):
    size_b, size_x, cap = dims
    tok_dev, width = tok_rows.shape
    slots = 2 * size_b * size_x * cap
    rows, slot_rows, parts = tok_dev // LANES, slots // LANES, width // LANES
    vmem, hbm = pl.BlockSpec(memory_space=pltpu.VMEM), pl.BlockSpec(memory_space=pltpu.HBM)
    return pl.pallas_call(
        functools.partial(dispatch_kernel, dims),
        name="dispatch",
        out_shape=(jax.ShapeDtypeStruct((slots, width), BF16), jax.ShapeDtypeStruct((rows, LANES), jnp.int32)),
        in_specs=[vmem, vmem, hbm],
        out_specs=(hbm, vmem),
        scratch_shapes=[
            pltpu.VMEM((tok_dev, width), BF16),
            pltpu.VMEM((tok_dev * parts, LANES), F32),
            pltpu.VMEM((slot_rows, LANES), jnp.int32),
            pltpu.SMEM((slot_rows, LANES), jnp.int32),
            pltpu.VMEM((LANES * parts, LANES), F32),
            pltpu.VMEM((4, LANES, width), BF16),
            pltpu.SemaphoreType.DMA,
            pltpu.SemaphoreType.DMA,
            pltpu.SemaphoreType.DMA((4,)),
        ],
        compiler_params=pltpu.CompilerParams(vmem_limit_bytes=40 << 20),
        cost_estimate=pl.CostEstimate(flops=20_000_000_000, bytes_accessed=15_000_000, transcendentals=0),
    )(ids.reshape(rows, LANES), order.reshape(rows, LANES), tok_rows)


def peers(dims, pos_x, pos_y, core):
    size_b, size_x, _ = dims

    def sends_to(kind, k):
        return (pos_y, 2 * k) if kind == 0 else (k, 2 * pos_x + 1)

    def serves(k, c):
        return (core * k + (1 - core) * pos_y, 2 * (core * pos_x + (1 - core) * k) + c)

    return sends_to, serves


def exchange_kernel(dims, send_hbm, *refs):
    size_b, size_x, cap = dims
    n = size_x
    w1_hbm, w2_hbm = refs[:n], refs[n:2 * n]
    b1_ref, b2_ref, back_hbm, w1, w2, recv, result, w_sem, out_sem, in_sem, ret_sem, back_sem = refs[2 * n:]
    i_b, i_a = lax.axis_index("ep_b"), lax.axis_index("ep_a")
    i_dp = lax.axis_index("dp")
    pos_x, core, pos_y = i_a // 2, lax.rem(i_a, 2), i_b
    pos = (1 - core) * pos_x + core * pos_y
    wpos = (1 - core) * pos_y + core * pos_x
    sends_to, serves = peers(dims, pos_x, pos_y, core)

    w_copies = []
    for d in range(n):
        w_copies.append(pltpu.make_async_copy(w1_hbm[d], w1.at[pl.ds(d, 1)], w_sem.at[0, d]))
        w_copies.append(pltpu.make_async_copy(w2_hbm[d], w2.at[pl.ds(d, 1)], w_sem.at[1, d]))
    for copy in w_copies:
        copy.start()

    barrier = pltpu.get_barrier_semaphore()
    for k in range(n):
        for c in range(2):
            for b, a in (sends_to(c, k), serves(k, c)):
                pl.semaphore_signal(barrier, inc=1, device_id=(i_dp, b, a), device_id_type=MESH_ID)
    pl.semaphore_wait(barrier, 4 * n)

    def out_copy(kind, step, j):
        my_place = pos_x if kind == 0 else pos_y
        k = lax.rem(my_place + step, n)
        b, a = sends_to(kind, k)
        src = (kind * n + k) * n + j
        dst = (my_place * n + j) * 2 + core
        return pltpu.make_async_remote_copy(
            src_ref=send_hbm.at[pl.ds(pl.multiple_of(src * cap, cap), cap)],
            dst_ref=recv.at[pl.ds(pl.multiple_of(dst * cap, cap), cap)],
            send_sem=out_sem.at[(kind * n + step) * n + j],
            recv_sem=in_sem.at[dst],
            device_id=(i_dp, b, a), device_id_type=MESH_ID)

    def ret_copy(k, j, c):
        b, a = serves(k, c)
        src = (k * n + j) * 2 + c
        dst = (core * n + pos) * n + j
        return pltpu.make_async_remote_copy(
            src_ref=result.at[pl.ds(pl.multiple_of(src * cap, cap), cap)],
            dst_ref=back_hbm.at[pl.ds(pl.multiple_of(dst * cap, cap), cap)],
            send_sem=ret_sem.at[src],
            recv_sem=back_sem.at[dst],
            device_id=(i_dp, b, a), device_id_type=MESH_ID)

    def send_slots(kind, step, j):
        if step:
            out_copy(kind, step, j).start()
            return

        @pl.when(kind != core)
        def _():
            out_copy(kind, step, j).start()

        @pl.when(kind == core)
        def _():
            own_slots(j).start()

    def own_slots(j):
        src, dst = (core * n + pos) * n + j, (pos * n + j) * 2 + core
        return pltpu.make_async_copy(send_hbm.at[pl.ds(pl.multiple_of(src * cap, cap), cap)],
                                     recv.at[pl.ds(pl.multiple_of(dst * cap, cap), cap)], in_sem.at[dst])

    def own_results(j):
        src, dst = (pos * n + j) * 2 + core, (core * n + pos) * n + j
        return pltpu.make_async_copy(result.at[pl.ds(pl.multiple_of(src * cap, cap), cap)],
                                     back_hbm.at[pl.ds(pl.multiple_of(dst * cap, cap), cap)], back_sem.at[dst])

    steps = [0, 1, n - 1] + list(range(2, n - 1))
    for group in ([0], [1, n - 1], list(range(2, n - 1))):
        for j in range(n):
            for step in group:
                for kind in range(2):
                    send_slots(kind, step, j)

    for copy in w_copies:
        copy.wait()

    def place(t):
        order = jnp.int32(0)
        for i, step in enumerate(steps):
            order = order + jnp.where(t // n == i, step, 0)
        k = lax.rem(pos - order + n, n)
        off = lax.rem(t, n)
        return k, off, lax.rem(wpos + off, n)

    def send_results(t):
        k, _, j = place(t)
        for c in range(2):
            mine = (k == pos) & (core == c)

            @pl.when(mine)
            def _():
                own_results(j).start()

            @pl.when(jnp.logical_not(mine))
            def _(c=c):
                ret_copy(k, j, c).start()

    def serve(t, _):
        k, off, j = place(t)
        first = (k * n + j) * 2
        for c in range(2):
            pltpu.make_async_remote_copy(
                src_ref=send_hbm.at[pl.ds(0, cap)],
                dst_ref=recv.at[pl.ds(pl.multiple_of((first + c) * cap, cap), cap)],
                send_sem=out_sem.at[0], recv_sem=in_sem.at[first + c],
                device_id=(i_dp, i_b, i_a), device_id_type=MESH_ID).wait_recv()
        rows = pl.ds(pl.multiple_of(first * cap, 2 * cap), 2 * cap)
        x = recv[rows, :]
        hidden = jnp.dot(x, w1[off], preferred_element_type=F32) + b1_ref[off].astype(F32)
        hidden = (0.5 * hidden * (1.0 + lax.erf(hidden * (0.5 ** 0.5)))).astype(BF16)
        y = jnp.dot(hidden, w2[off], preferred_element_type=F32) + b2_ref[off].astype(F32)
        result[rows, :] = y.astype(BF16)

        @pl.when(t > 0)
        def _():
            send_results(t - 1)
        return 0

    blocks = n * n
    lax.fori_loop(0, blocks, serve, 0)
    send_results(jnp.int32(blocks - 1))

    def drain(t, _):
        block = pl.ds(pl.multiple_of(t * cap, cap), cap)
        kind, step = t // (n * n), lax.rem(t // n, n)
        sent = pltpu.make_async_remote_copy(
            src_ref=send_hbm.at[block], dst_ref=recv.at[block],
            send_sem=out_sem.at[t], recv_sem=in_sem.at[t],
            device_id=(i_dp, i_b, i_a), device_id_type=MESH_ID)
        returned = pltpu.make_async_remote_copy(
            src_ref=result.at[block], dst_ref=back_hbm.at[block],
            send_sem=ret_sem.at[t], recv_sem=back_sem.at[t],
            device_id=(i_dp, i_b, i_a), device_id_type=MESH_ID)

        @pl.when((kind != core) | (step != 0))
        def _():
            sent.wait_send()

        @pl.when((t // (2 * n) != pos) | (lax.rem(t, 2) != core))
        def _():
            returned.wait_send()

        returned.wait_recv()
        return 0

    lax.fori_loop(0, 2 * blocks, drain, 0)


def exchange(send_rows, w1, b1, w2, b2, dims):
    size_b, size_x, cap = dims
    n = size_x
    slots, width = send_rows.shape
    hidden = w1[0].shape[2]
    vmem, hbm = pl.BlockSpec(memory_space=pltpu.VMEM), pl.BlockSpec(memory_space=pltpu.HBM)
    return pl.pallas_call(
        functools.partial(exchange_kernel, dims),
        name="exchange",
        out_shape=jax.ShapeDtypeStruct((slots, width), BF16),
        in_specs=[pl.BlockSpec(memory_space=pl.ANY)] + [hbm] * (2 * n) + [vmem] * 2,
        out_specs=hbm,
        scratch_shapes=[
            pltpu.VMEM((n, width, hidden), BF16),
            pltpu.VMEM((n, hidden, width), BF16),
            pltpu.VMEM((slots, width), BF16),
            pltpu.VMEM((slots, width), BF16),
            pltpu.SemaphoreType.DMA((2, n)),
            pltpu.SemaphoreType.DMA((2 * n * n,)),
            pltpu.SemaphoreType.DMA((2 * n * n,)),
            pltpu.SemaphoreType.DMA((2 * n * n,)),
            pltpu.SemaphoreType.DMA((2 * n * n,)),
        ],
        compiler_params=pltpu.CompilerParams(collective_id=1, has_side_effects=True, vmem_limit_bytes=60 << 20),
        cost_estimate=pl.CostEstimate(flops=4 * slots * width * hidden, bytes_accessed=30_000_000, transcendentals=0),
    )(send_rows, *w1, *w2, b1, b2)


def combine_kernel(back_hbm, dest_sm, gate_sm, out_ref, stage, big, tmp, sem):
    i = pl.program_id(0)
    slots, width = back_hbm.shape
    parts = width // LANES
    chunk = stage.shape[1]
    chunks = slots // chunk

    @pl.when(i == 0)
    def _():
        def fetch(q):
            return pltpu.make_async_copy(back_hbm.at[pl.ds(pl.multiple_of(q * chunk, chunk), chunk)], stage.at[lax.rem(q, 2)],
                                         sem.at[lax.rem(q, 2)])
        fetch(0).start()
        big[pl.ds(slots * parts, 8), :] = jnp.zeros((8, LANES), F32)

        def widen_chunk(q, _):
            @pl.when(q + 1 < chunks)
            def _():
                fetch(q + 1).start()
            fetch(q).wait()

            def widen(u, _):
                base = pl.multiple_of(u * 16, 16)
                for c in range(parts):
                    big[pl.ds((q * chunk + base) * parts + c, 16, stride=parts), :] = (
                        stage[lax.rem(q, 2), pl.ds(base, 16), c * LANES:(c + 1) * LANES].astype(F32))
                return 0

            lax.fori_loop(0, chunk // 16, widen, 0, unroll=8)
            return 0

        lax.fori_loop(0, chunks, widen_chunk, 0)

    def gather(g, _):
        row = i * (out_ref.shape[0] // LANES) + g
        for j in range(LANES):
            tmp[pl.ds(j * parts, parts), :] = big[pl.ds(dest_sm[row, j], parts), :] * gate_sm[row, j]
        for j in range(0, LANES, 16):
            for c in range(parts):
                out_ref[pl.ds(pl.multiple_of(g * LANES + j, 16), 16), c * LANES:(c + 1) * LANES] = (
                    tmp[pl.ds(j * parts + c, 16, stride=parts), :].astype(BF16))
        return 0

    lax.fori_loop(0, out_ref.shape[0] // LANES, gather, 0)


def combine(back_rows, dest, gate, tok_dev):
    slots, width = back_rows.shape
    parts = width // LANES
    block = 1024
    smem = pl.BlockSpec(memory_space=pltpu.SMEM)
    return pl.pallas_call(
        combine_kernel,
        name="combine",
        grid=(tok_dev // block,),
        out_shape=jax.ShapeDtypeStruct((tok_dev, width), BF16),
        in_specs=[pl.BlockSpec(memory_space=pltpu.HBM), smem, smem],
        out_specs=pl.BlockSpec((block, width), lambda i: (i, 0)),
        scratch_shapes=[
            pltpu.VMEM((2, 1280, width), BF16),
            pltpu.VMEM((slots * parts + 8, LANES), F32),
            pltpu.VMEM((LANES * parts, LANES), F32),
            pltpu.SemaphoreType.DMA((2,)),
        ],
        compiler_params=pltpu.CompilerParams(vmem_limit_bytes=40 << 20, dimension_semantics=("arbitrary",)),
        cost_estimate=pl.CostEstimate(flops=20_000_000_000, bytes_accessed=15_000_000, transcendentals=0),
    )(back_rows, dest, gate)


def gates(tok_rows, id_row, w_route, expert_keys, temperature):
    num_experts = expert_keys.shape[0]
    keys_f32 = expert_keys.astype(F32)
    key_unit = keys_f32 / jnp.sqrt(jnp.sum(keys_f32 * keys_f32, axis=1, keepdims=True))
    projected = jnp.dot(tok_rows, w_route, preferred_element_type=F32)
    proj_unit = projected / jnp.sqrt(jnp.sum(projected * projected, axis=1, keepdims=True))
    router_prob = jax.nn.softmax(jnp.dot(proj_unit, key_unit.T) / temperature, axis=1)
    expert_range = jnp.arange(num_experts, dtype=jnp.int32)[None, :]
    return jnp.sum(jnp.where(id_row[:, None] == expert_range, router_prob, 0.0), axis=1)


def solution(mesh):
    size_b, size_x = mesh.shape["ep_b"], mesh.shape["ep_a"] // 2
    num_experts = 2 * size_b * size_x
    tok_spec = P(("dp",) + EXPERT_AXES)
    expert_spec = P(EXPERT_AXES)

    def share(w):
        out = [w]
        for d in range(1, size_x):
            pairs = []
            for y in range(size_b):
                for x in range(size_x):
                    pairs.append(((y * size_x + x) * 2, (((y - d) % size_b) * size_x + x) * 2))
                    pairs.append(((y * size_x + x) * 2 + 1, (y * size_x + (x - d) % size_x) * 2 + 1))
            out.append(lax.ppermute(w, EXPERT_AXES, pairs))
        return out

    def device_step(tokens, expert_ids, route_order, w_route, expert_keys, temperature, w_in, b_in, w_out, b_out):
        tok_dev = tokens.shape[1]
        cap = (5 * tok_dev + 4 * num_experts - 1) // (4 * num_experts)
        dims = (size_b, size_x, cap)
        w1, w2 = share(w_in), share(w_out)
        b1, b2 = (jnp.concatenate(share(b[:, None, :]), axis=0) for b in (b_in, b_out))
        send_rows, dest = dispatch(tokens[0], expert_ids[0], route_order[0], dims)
        gate = gates(tokens[0], expert_ids[0], w_route, expert_keys, temperature).reshape(tok_dev // LANES, LANES)
        back_rows = exchange(send_rows, w1, b1, w2, b2, dims)
        return combine(back_rows, dest, gate, tok_dev)[None]

    return jax.shard_map(
        device_step,
        mesh=mesh,
        in_specs=(tok_spec, tok_spec, tok_spec, P(), P(), P(), expert_spec, expert_spec, expert_spec, expert_spec),
        out_specs=tok_spec,
        check_vma=False,
    )
```

```python
import functools

import jax
import jax.numpy as jnp
from jax import lax
from jax.experimental import pallas as pl
from jax.experimental.pallas import tpu as pltpu
from jax.sharding import PartitionSpec as P

EXPERT_AXES = ("ep_b", "ep_a")
LANES = 128
MESH_ID = pl.DeviceIdType.MESH
F32 = jnp.float32
BF16 = jnp.bfloat16


def iota(shape, dim):
    return lax.broadcasted_iota(jnp.int32, shape, dim)


def dot_nt(a, b):
    return lax.dot_general(a, b, (((1,), (1,)), ((), ())), preferred_element_type=F32)


def as_bf16(mask):
    return jnp.where(mask, 1.0, 0.0).astype(BF16)


def virtual_expert(ids, size_b, size_x):
    i_b, i_a = ids // (2 * size_x), ids % (2 * size_x)
    x, core = i_a // 2, i_a % 2
    return jnp.where(core == 0, x * size_b + i_b, size_b * size_x + i_b * size_x + x)


def route_kernel(dims, parts, ids_ref, order_ref, src_ref, dest_ref):
    size_b, size_x, cap = dims
    rows, slot_rows = ids_ref.shape[0], src_ref.shape[0]
    num_experts = 2 * size_b * size_x
    upper = as_bf16((iota((LANES, 2 * LANES), 0) <= iota((LANES, 2 * LANES), 1)) | (iota((LANES, 2 * LANES), 1) >= LANES))
    ids_t = ids_ref[...].astype(F32).T.astype(BF16)
    iota_rows = iota((rows, LANES), 0)
    iota_lane = iota((LANES, LANES), 0)
    iota_exp = iota((num_experts, LANES), 0)

    def ranked(r, carry):
        count, keep = carry
        o = order_ref[pl.ds(r, 1), :]
        pick_hi = iota_rows == o // LANES
        pick_lo = iota_lane == o % LANES
        table = jnp.dot(ids_t, as_bf16(pick_hi), preferred_element_type=F32)
        rid = jnp.sum(jnp.where(pick_lo, table, 0.0), axis=0, keepdims=True)
        mine = iota_exp.astype(F32) == rid
        both = jnp.dot(as_bf16(mine), upper, preferred_element_type=F32)
        rank = jnp.sum(jnp.where(mine, both[:, :LANES] + count, 0.0), axis=0, keepdims=True)
        keep = keep + dot_nt(as_bf16(pick_hi & (rank <= float(cap))), as_bf16(pick_lo))
        return count + both[:, LANES:], keep

    zero_count = jnp.zeros((num_experts, LANES), F32)
    _, keep = lax.fori_loop(0, rows, ranked, (zero_count, jnp.zeros((rows, LANES), F32)), unroll=8)
    dest_ref[...] = keep.astype(jnp.int32)

    iota_slot = iota((slot_rows, LANES), 0)
    lane = iota((1, LANES), 1).astype(F32)

    def placed(r, carry):
        count, source = carry
        expert = virtual_expert(ids_ref[pl.ds(r, 1), :], size_b, size_x)
        kept = dest_ref[pl.ds(r, 1), :] > 0
        mine = (iota_exp == expert) & kept
        both = jnp.dot(as_bf16(mine), upper, preferred_element_type=F32)
        place = jnp.sum(jnp.where(mine, both[:, :LANES] + count, 0.0), axis=0, keepdims=True) - 1.0
        slot = jnp.where(kept, expert * cap + place.astype(jnp.int32), num_experts * cap)
        dest_ref[pl.ds(r, 1), :] = slot * parts
        hit = jnp.where(iota_slot == slot // LANES, 1.0, 0.0)
        stacked = jnp.concatenate([hit * lax.convert_element_type(r, F32), hit * lane], axis=0).astype(BF16)
        source = source + dot_nt(stacked, as_bf16(iota_lane == slot % LANES))
        return count + both[:, LANES:], source

    _, source = lax.fori_loop(0, rows, placed, (zero_count, jnp.zeros((2 * slot_rows, LANES), F32)), unroll=4)
    src_ref[...] = ((source[:slot_rows] * float(LANES) + source[slot_rows:]) * float(parts)).astype(jnp.int32)


def route(ids, order, dims, parts):
    size_b, size_x, cap = dims
    slot_rows = 2 * size_b * size_x * cap // LANES
    return pl.pallas_call(
        functools.partial(route_kernel, dims, parts),
        name="route",
        out_shape=(jax.ShapeDtypeStruct((slot_rows, LANES), jnp.int32), jax.ShapeDtypeStruct(ids.shape, jnp.int32)),
        cost_estimate=pl.CostEstimate(flops=5_000_000_000, bytes_accessed=200_000, transcendentals=0),
    )(ids, order)


def pick(table, t):
    value = jnp.int32(0)
    for i, entry in enumerate(table):
        if entry:
            value = value + jnp.where(t == i, entry, 0)
    return value


def experts_kernel(dims, ids_ref, src_sm, wr_ref, keys_ref, tau_ref, bias_hbm, tok_hbm, w1_hbm, w2_hbm,
                   back_hbm, gate_ref,
                   tok_vm, big, tmp, send, recv, w1, w2, bias,
                   tok_sem, wout_sem, win_sem, out_sem, in_sem, ret_sem, back_sem):
    size_b, size_x, cap = dims
    n = size_x
    rows = ids_ref.shape[0]
    num_experts = 2 * size_b * size_x
    parts = tok_vm.shape[1] // LANES
    i_dp, i_b, i_a = lax.axis_index("dp"), lax.axis_index("ep_b"), lax.axis_index("ep_a")
    pos_x, core, pos_y = i_a // 2, lax.rem(i_a, 2), i_b
    pos = (1 - core) * pos_x + core * pos_y
    wpos = (1 - core) * pos_y + core * pos_x

    def sends_to(kind, k):
        return i_dp, (1 - kind) * pos_y + kind * k, 2 * ((1 - kind) * k + kind * pos_x) + kind

    def serves(k, c):
        return i_dp, core * k + (1 - core) * pos_y, 2 * (core * pos_x + (1 - core) * k) + c

    def shares(k):
        return i_dp, (1 - core) * k + core * pos_y, 2 * ((1 - core) * pos_x + core * k) + core

    def block(i):
        return pl.ds(pl.multiple_of(i * cap, cap), cap)

    tok_copy = pltpu.make_async_copy(tok_hbm, tok_vm, tok_sem)
    tok_copy.start()
    held = ((w1_hbm, w1), (w2_hbm, w2), (bias_hbm, bias))
    for i, (own, every) in enumerate(held):
        pltpu.make_async_copy(own, every.at[pl.ds(0, 1)], win_sem.at[i, 0]).start()

    barrier = pltpu.get_barrier_semaphore()
    for k in range(n):
        for c in range(2):
            for device in (sends_to(c, k), serves(k, c)):
                pl.semaphore_signal(barrier, inc=1, device_id=device, device_id_type=MESH_ID)
    for d in range(1, n):
        pl.semaphore_signal(barrier, inc=1, device_id=shares(lax.rem(wpos + d, n)), device_id_type=MESH_ID)
    pl.semaphore_wait(barrier, 5 * n - 1)

    def weight_copy(i, d):
        own, every = held[i]
        return pltpu.make_async_remote_copy(
            src_ref=own, dst_ref=every.at[pl.ds(d, 1)], send_sem=wout_sem.at[i, d], recv_sem=win_sem.at[i, d],
            device_id=shares(lax.rem(wpos - d + n, n)), device_id_type=MESH_ID)

    weight_order = [1, n - 1] + list(range(2, n - 1))
    for d in weight_order:
        for i in (2, 0, 1):
            weight_copy(i, d).start()

    iota_exp = iota((num_experts, LANES), 0)

    tok_copy.wait()

    def widen(i, _):
        base = pl.multiple_of(i * 16, 16)
        for c in range(parts):
            big[pl.ds(base * parts + c, 16, stride=parts), :] = tok_vm[pl.ds(base, 16), c * LANES:(c + 1) * LANES].astype(F32)
        return 0

    lax.fori_loop(0, tok_vm.shape[0] // 16, widen, 0, unroll=8)

    near, far = [1, n - 1], list(range(2, n - 1))
    send_order = [(step, off, kind) for group in (near, far, [0]) for off in range(n) for step in group for kind in range(2)]

    def outgoing(t):
        step, off, kind = (pick([e[i] for e in send_order], t) for i in range(3))
        k = lax.rem((1 - kind) * pos_x + kind * pos_y + step, n)
        j = lax.rem((1 - kind) * pos_y + kind * pos_x + off, n)
        return step, kind, k, j

    def send_block(t):
        step, kind, k, j = outgoing(t)
        src = (kind * n + k) * n + j
        dst = (((1 - kind) * pos_x + kind * pos_y) * n + j) * 2 + core
        own = (step == 0) & (kind == core)

        @pl.when(own)
        def _():
            pltpu.make_async_copy(send.at[block(src)], recv.at[block(dst)], in_sem.at[dst]).start()

        @pl.when(jnp.logical_not(own))
        def _():
            pltpu.make_async_remote_copy(
                src_ref=send.at[block(src)], dst_ref=recv.at[block(dst)], send_sem=out_sem.at[src], recv_sem=in_sem.at[dst],
                device_id=sends_to(kind, k), device_id_type=MESH_ID).start()

    group_rows = 64 if cap % 64 == 0 else 16

    def gather_block(t, _):
        _, kind, k, j = outgoing(t)
        base = ((kind * n + k) * n + j) * cap

        def gather(g, _):
            first = pl.multiple_of(base + g * group_rows, group_rows)
            row, col = first // LANES, lax.rem(first, LANES)
            for u in range(group_rows):
                tmp[pl.ds(u * parts, parts), :] = big[pl.ds(src_sm[row, col + u], parts), :]
            for u in range(0, group_rows, 16):
                for c in range(parts):
                    send[pl.ds(pl.multiple_of(first + u, 16), 16), c * LANES:(c + 1) * LANES] = (
                        tmp[pl.ds(u * parts + c, 16, stride=parts), :].astype(BF16))
            return 0

        lax.fori_loop(0, cap // group_rows, gather, 0)

        @pl.when(t > 0)
        def _():
            send_block(t - 1)
        return 0

    blocks = 2 * n * n
    lax.fori_loop(0, blocks, gather_block, 0)

    keys = keys_ref[...].astype(F32)
    key_unit = keys / jnp.sqrt(jnp.sum(keys * keys, axis=1, keepdims=True))
    tau = tau_ref[0, 0]
    ones = jnp.ones((8, wr_ref.shape[1]), F32)
    span = 4

    def gate_rows(i, _):
        x = tok_vm[pl.ds(pl.multiple_of(i * span * LANES, span * LANES), span * LANES), :]
        r = jnp.dot(x, wr_ref[...], preferred_element_type=F32)
        exact = dict(preferred_element_type=F32, precision=lax.Precision.HIGHEST)
        dots = lax.dot_general(key_unit, r, (((1,), (1,)), ((), ())), **exact)
        norm = jnp.sqrt(lax.dot_general(ones, r * r, (((1,), (1,)), ((), ())), **exact)[:1])
        logits = dots / norm / tau
        p = jnp.exp(logits - jnp.max(logits, axis=0, keepdims=True))
        total = jnp.sum(p, axis=0, keepdims=True)
        for q in range(span):
            mine = iota_exp == ids_ref[pl.ds(i * span + q, 1), :]
            cols = slice(q * LANES, (q + 1) * LANES)
            gate_ref[pl.ds(i * span + q, 1), :] = jnp.sum(jnp.where(mine, p[:, cols], 0.0), axis=0, keepdims=True) / total[:, cols]
        return 0

    send_block(jnp.int32(blocks - 1))
    lax.fori_loop(0, rows // span, gate_rows, 0)

    serve_order = ([(0, off) for off in range(n // 2)] + [(step, off) for off in range(n) for step in near]
                   + [(0, off) for off in range(n // 2, n - 1)] + [(step, off) for step in far for off in range(n)] + [(0, n - 1)])
    first_use = [int(off not in [o for _, o in serve_order[:i]]) for i, (_, off) in enumerate(serve_order)]

    def incoming(t):
        step, off = (pick([e[i] for e in serve_order], t) for i in range(2))
        return lax.rem(pos - step + n, n), off, lax.rem(wpos + off, n)

    def result_ends(t, c):
        k, _, j = incoming(t)
        src, dst = (k * n + j) * 2 + c, (core * n + pos) * n + j
        return k, src, dst, (k == pos) & (core == c)

    def send_results(t):
        for c in range(2):
            k, src, dst, own = result_ends(t, c)

            @pl.when(own)
            def _():
                pltpu.make_async_copy(recv.at[block(src)], back_hbm.at[block(dst)], back_sem.at[dst]).start()

            @pl.when(jnp.logical_not(own))
            def _():
                pltpu.make_async_remote_copy(
                    src_ref=recv.at[block(src)], dst_ref=back_hbm.at[block(dst)], send_sem=ret_sem.at[src],
                    recv_sem=back_sem.at[dst], device_id=serves(k, c), device_id_type=MESH_ID).start()

    def serve(t, _):
        k, off, j = incoming(t)
        first = (k * n + j) * 2

        @pl.when(pick(first_use, t) == 1)
        def _():
            for i, (own, every) in enumerate(held):
                pltpu.make_async_copy(own, every.at[pl.ds(off, 1)], win_sem.at[i, off]).wait()

        for c in range(2):
            pltpu.make_async_copy(send.at[block(0)], recv.at[block(first + c)], in_sem.at[first + c]).wait()
        here = pl.ds(pl.multiple_of(first * cap, 2 * cap), 2 * cap)
        hidden = jnp.dot(recv[here, :], w1[off], preferred_element_type=F32) + bias[off, 0:1, :].astype(F32)
        hidden = (0.5 * hidden * (1.0 + lax.erf(hidden * (0.5 ** 0.5)))).astype(BF16)
        y = jnp.dot(hidden, w2[off], preferred_element_type=F32) + bias[off, 1:2, :recv.shape[1]].astype(F32)
        recv[here, :] = y.astype(BF16)

        @pl.when(t > 0)
        def _():
            send_results(t - 1)
        return 0

    lax.fori_loop(0, n * n, serve, 0)
    send_results(jnp.int32(n * n - 1))

    for d in range(1, n):
        for i in range(3):
            weight_copy(i, d).wait_send()

    def drain(t, _):
        sent = pltpu.make_async_remote_copy(
            src_ref=send.at[block(t)], dst_ref=recv.at[block(t)], send_sem=out_sem.at[t], recv_sem=in_sem.at[t],
            device_id=(i_dp, i_b, i_a), device_id_type=MESH_ID)
        returned = pltpu.make_async_remote_copy(
            src_ref=recv.at[block(t)], dst_ref=back_hbm.at[block(t)], send_sem=ret_sem.at[t], recv_sem=back_sem.at[t],
            device_id=(i_dp, i_b, i_a), device_id_type=MESH_ID)
        kind, k = t // (n * n), lax.rem(t // n, n)

        @pl.when((kind != core) | (k != pos))
        def _():
            sent.wait_send()

        @pl.when((t // (2 * n) != pos) | (lax.rem(t, 2) != core))
        def _():
            returned.wait_send()

        returned.wait_recv()
        return 0

    lax.fori_loop(0, blocks, drain, 0)


def experts(tok_rows, ids, source, w_route, expert_keys, temperature, w1, w2, bias, dims):
    size_b, size_x, cap = dims
    n = size_x
    tok_dev, width = tok_rows.shape
    hidden = w1.shape[2]
    slots = 2 * size_b * size_x * cap
    rows, parts = tok_dev // LANES, width // LANES
    vmem, smem, hbm = (pl.BlockSpec(memory_space=m) for m in (pltpu.VMEM, pltpu.SMEM, pltpu.HBM))
    dma = pltpu.SemaphoreType.DMA
    return pl.pallas_call(
        functools.partial(experts_kernel, dims),
        name="experts",
        out_shape=(jax.ShapeDtypeStruct((slots, width), BF16), jax.ShapeDtypeStruct((rows, LANES), F32)),
        in_specs=[vmem, smem, vmem, vmem, smem] + [hbm] * 4,
        out_specs=(hbm, vmem),
        scratch_shapes=[
            pltpu.VMEM((tok_dev, width), BF16),
            pltpu.VMEM((tok_dev * parts + 8, LANES), F32),
            pltpu.VMEM((64 * parts + 8, LANES), F32),
            pltpu.VMEM((slots, width), BF16),
            pltpu.VMEM((slots, width), BF16),
            pltpu.VMEM((n, width, hidden), BF16),
            pltpu.VMEM((n, hidden, width), BF16),
            pltpu.VMEM((n,) + bias.shape[1:], BF16),
            dma, dma((3, n)), dma((3, n)),
            dma((2 * n * n,)), dma((2 * n * n,)), dma((2 * n * n,)), dma((2 * n * n,)),
        ],
        compiler_params=pltpu.CompilerParams(collective_id=1, has_side_effects=True, vmem_limit_bytes=60 << 20),
        cost_estimate=pl.CostEstimate(flops=4 * slots * width * hidden, bytes_accessed=30_000_000, transcendentals=0),
    )(ids, source, w_route, expert_keys, temperature.reshape(1, 1),
      bias, tok_rows, w1, w2)


def combine_kernel(back_hbm, dest_sm, gate_sm, out_ref, stage, big, tmp, sem):
    i = pl.program_id(0)
    slots, width = back_hbm.shape
    parts = width // LANES
    chunk = stage.shape[1]
    chunks = slots // chunk

    @pl.when(i == 0)
    def _():
        def fetch(q):
            return pltpu.make_async_copy(back_hbm.at[pl.ds(pl.multiple_of(q * chunk, chunk), chunk)], stage.at[lax.rem(q, 2)],
                                         sem.at[lax.rem(q, 2)])
        fetch(0).start()
        big[pl.ds(slots * parts, 8), :] = jnp.zeros((8, LANES), F32)

        def widen_chunk(q, _):
            @pl.when(q + 1 < chunks)
            def _():
                fetch(q + 1).start()
            fetch(q).wait()

            def widen(u, _):
                base = pl.multiple_of(u * 16, 16)
                for c in range(parts):
                    big[pl.ds((q * chunk + base) * parts + c, 16, stride=parts), :] = (
                        stage[lax.rem(q, 2), pl.ds(base, 16), c * LANES:(c + 1) * LANES].astype(F32))
                return 0

            lax.fori_loop(0, chunk // 16, widen, 0, unroll=8)
            return 0

        lax.fori_loop(0, chunks, widen_chunk, 0)

    def gather(g, _):
        row = i * (out_ref.shape[0] // LANES) + g
        for j in range(LANES):
            tmp[pl.ds(j * parts, parts), :] = big[pl.ds(dest_sm[row, j], parts), :] * gate_sm[row, j]
        for j in range(0, LANES, 16):
            for c in range(parts):
                out_ref[pl.ds(pl.multiple_of(g * LANES + j, 16), 16), c * LANES:(c + 1) * LANES] = (
                    tmp[pl.ds(j * parts + c, 16, stride=parts), :].astype(BF16))
        return 0

    lax.fori_loop(0, out_ref.shape[0] // LANES, gather, 0)


def combine(back_rows, dest, gate, tok_dev):
    slots, width = back_rows.shape
    parts = width // LANES
    block = 1024
    smem = pl.BlockSpec(memory_space=pltpu.SMEM)
    return pl.pallas_call(
        combine_kernel,
        name="combine",
        grid=(tok_dev // block,),
        out_shape=jax.ShapeDtypeStruct((tok_dev, width), BF16),
        in_specs=[pl.BlockSpec(memory_space=pltpu.HBM), smem, smem],
        out_specs=pl.BlockSpec((block, width), lambda i: (i, 0)),
        scratch_shapes=[
            pltpu.VMEM((2, 1280, width), BF16),
            pltpu.VMEM((slots * parts + 8, LANES), F32),
            pltpu.VMEM((LANES * parts, LANES), F32),
            pltpu.SemaphoreType.DMA((2,)),
        ],
        compiler_params=pltpu.CompilerParams(vmem_limit_bytes=40 << 20, dimension_semantics=("arbitrary",)),
        cost_estimate=pl.CostEstimate(flops=20_000_000_000, bytes_accessed=15_000_000, transcendentals=0),
    )(back_rows, dest, gate)


def solution(mesh):
    size_b, size_x = mesh.shape["ep_b"], mesh.shape["ep_a"] // 2
    num_experts = 2 * size_b * size_x
    tok_spec = P(("dp",) + EXPERT_AXES)
    expert_spec = P(EXPERT_AXES)

    def device_step(tokens, expert_ids, route_order, w_route, expert_keys, temperature, w_in, b_in, w_out, b_out):
        tok_dev = tokens.shape[1]
        cap = (5 * tok_dev + 4 * num_experts - 1) // (4 * num_experts)
        dims = (size_b, size_x, cap)
        widen = lambda b: jnp.pad(b, ((0, 0), (0, w_in.shape[2] - b.shape[1])))
        bias = jnp.pad(jnp.stack([b_in, widen(b_out)], axis=1), ((0, 0), (0, 14), (0, 0)))
        ids = expert_ids.reshape(tok_dev // LANES, LANES)
        source, dest = route(ids, route_order.reshape(ids.shape), dims, tokens.shape[2] // LANES)
        back_rows, gate = experts(tokens[0], ids, source, w_route, expert_keys, temperature, w_in, w_out, bias, dims)
        return combine(back_rows, dest, gate, tok_dev)[None]

    return jax.shard_map(
        device_step,
        mesh=mesh,
        in_specs=(tok_spec, tok_spec, tok_spec, P(), P(), P(), expert_spec, expert_spec, expert_spec, expert_spec),
        out_specs=tok_spec,
        check_vma=False,
    )
```

```python
import functools

import jax
import jax.numpy as jnp
from jax import lax
from jax.experimental import pallas as pl
from jax.experimental.pallas import tpu as pltpu
from jax.sharding import PartitionSpec as P

EXPERT_AXES = ("ep_b", "ep_a")
LANES = 128
MESH_ID = pl.DeviceIdType.MESH
F32 = jnp.float32
BF16 = jnp.bfloat16


def iota(shape, dim):
    return lax.broadcasted_iota(jnp.int32, shape, dim)


def dot_nt(a, b):
    return lax.dot_general(a, b, (((1,), (1,)), ((), ())), preferred_element_type=F32)


def as_bf16(mask):
    return jnp.where(mask, 1.0, 0.0).astype(BF16)


def virtual_expert(ids, size_b, size_x):
    i_b, i_a = ids // (2 * size_x), ids % (2 * size_x)
    x, core = i_a // 2, i_a % 2
    return jnp.where(core == 0, x * size_b + i_b, size_b * size_x + i_b * size_x + x)


def dispatch_kernel(dims, ids_ref, order_ref, tok_hbm, send_hbm, dest_ref,
                    rid_s, both_s, kept_s, hi_s, lo_s, src_vm, src_sm, tok_vm, big, tmp, send, tok_sem, src_sem, out_sem):
    size_b, size_x, cap = dims
    rows, slot_rows = ids_ref.shape[0], src_vm.shape[0]
    parts = tok_hbm.shape[1] // LANES
    tok_copy = pltpu.make_async_copy(tok_hbm, tok_vm, tok_sem)
    tok_copy.start()
    num_experts = 2 * size_b * size_x
    per_expert = slot_rows // num_experts
    upper = as_bf16((iota((LANES, 2 * LANES), 0) <= iota((LANES, 2 * LANES), 1)) | (iota((LANES, 2 * LANES), 1) >= LANES))
    ids_t = ids_ref[...].astype(F32).T.astype(BF16)
    iota_rows = iota((rows, LANES), 0)
    iota_lane = iota((LANES, LANES), 0)
    iota_exp = iota((num_experts, LANES), 0)
    iota_slot = iota((slot_rows, LANES), 0)
    zero_count = jnp.zeros((num_experts, LANES), F32)

    def row(r):
        return pl.ds(r, 1)

    def cols(r):
        return pl.ds(pl.multiple_of(r * LANES, LANES), LANES)

    def each(body, unroll):
        lax.fori_loop(0, rows, lambda r, _: (body(r), 0)[1], 0, unroll=unroll)

    def ranked_id(r):
        o = order_ref[row(r), :]
        table = jnp.dot(ids_t, as_bf16(iota_rows == o // LANES), preferred_element_type=F32)
        rid_s[row(r), :] = jnp.sum(jnp.where(iota_lane == o % LANES, table, 0.0), axis=0, keepdims=True).astype(jnp.int32)

    def ranked_count(r):
        both_s[r] = jnp.dot(as_bf16(iota_exp == rid_s[row(r), :]), upper, preferred_element_type=F32)

    def position(mine, r, count):
        return jnp.sum(jnp.where(mine, both_s[r, :, :LANES] + count, 0.0), axis=0, keepdims=True)

    def ranked_kept(r, count):
        rank = position(iota_exp == rid_s[row(r), :], r, count)
        kept_s[row(r), :] = (rank <= float(cap)).astype(jnp.int32)
        return count + both_s[r, :, LANES:]

    def scatter_kept(r):
        o = order_ref[row(r), :]
        hi_s[:rows, cols(r)] = as_bf16((iota_rows == o // LANES) & (kept_s[row(r), :] > 0))
        lo_s[:, cols(r)] = as_bf16(iota_lane == o % LANES)

    each(ranked_id, 16)
    each(ranked_count, 16)
    lax.fori_loop(0, rows, ranked_kept, zero_count, unroll=8)
    each(scatter_kept, 8)
    kept_s[...] = dot_nt(hi_s[:rows, :], lo_s[...]).astype(jnp.int32)

    def expert_of(r):
        return virtual_expert(ids_ref[row(r), :], size_b, size_x)

    def mine_kept(r):
        return (iota_exp == expert_of(r)) & (kept_s[row(r), :] > 0)

    def token_count(r):
        both_s[r] = jnp.dot(as_bf16(mine_kept(r)), upper, preferred_element_type=F32)

    lane = iota((1, LANES), 1).astype(F32)

    def placed(r, count):
        place = position(mine_kept(r), r, count).astype(jnp.int32) - 1
        kept = kept_s[row(r), :] > 0
        expert = expert_of(r)
        dest_ref[row(r), :] = jnp.where(kept, expert * cap + place, num_experts * cap) * parts
        rid_s[row(r), :] = jnp.where(kept, expert * (per_expert * LANES) + place, slot_rows * LANES)
        return count + both_s[r, :, LANES:]

    def scatter_source(r):
        slot = rid_s[row(r), :]
        hit = jnp.where(iota_slot == slot // LANES, 1.0, 0.0)
        hi_s[:slot_rows, cols(r)] = (hit * lax.convert_element_type(r, F32)).astype(BF16)
        hi_s[slot_rows:, cols(r)] = (hit * lane).astype(BF16)
        lo_s[:, cols(r)] = as_bf16(iota_lane == slot % LANES)

    each(token_count, 16)
    lax.fori_loop(0, rows, placed, zero_count, unroll=8)
    each(scatter_source, 8)
    found = dot_nt(hi_s[...], lo_s[...])
    src_vm[...] = ((found[:slot_rows] * float(LANES) + found[slot_rows:]) * float(parts)).astype(jnp.int32)
    src_copy = pltpu.make_async_copy(src_vm, src_sm, src_sem)
    src_copy.start()

    tok_copy.wait()

    def widen(i, _):
        base = pl.multiple_of(i * 16, 16)
        for c in range(parts):
            big[pl.ds(base * parts + c, 16, stride=parts), :] = tok_vm[pl.ds(base, 16), c * LANES:(c + 1) * LANES].astype(F32)
        return 0

    lax.fori_loop(0, tok_vm.shape[0] // 16, widen, 0, unroll=8)
    src_copy.wait()

    def gather_rows(row_index, first, count):
        for u in range(count):
            tmp[pl.ds(u * parts, parts), :] = big[pl.ds(src_sm[row_index, u], parts), :]
        for u in range(0, count, 16):
            for c in range(parts):
                send[pl.ds(pl.multiple_of(first + u, 16), 16), c * LANES:(c + 1) * LANES] = (
                    tmp[pl.ds(u * parts + c, 16, stride=parts), :].astype(BF16))

    def out_copy(index):
        rows_of = pl.ds(pl.multiple_of(index * cap, cap), cap)
        return pltpu.make_async_copy(send.at[rows_of], send_hbm.at[rows_of], out_sem)

    def gather_block(index, _):
        def gather(g, _):
            gather_rows(index * per_expert + g, pl.multiple_of(index * cap + g * LANES, 16), LANES)
            return 0

        lax.fori_loop(0, cap // LANES, gather, 0)
        if cap % LANES:
            gather_rows(index * per_expert + cap // LANES, pl.multiple_of(index * cap + cap // LANES * LANES, 16), cap % LANES)
        out_copy(index).start()
        return 0

    lax.fori_loop(0, num_experts, gather_block, 0)
    lax.fori_loop(0, num_experts, lambda index, _: (out_copy(index).wait(), 0)[1], 0)


def dispatch(tok_rows, ids, order, dims):
    size_b, size_x, cap = dims
    num_experts = 2 * size_b * size_x
    slots, slot_rows = num_experts * cap, num_experts * pl.cdiv(cap, LANES)
    tok_dev, width = tok_rows.shape
    rows, parts = tok_dev // LANES, width // LANES
    vmem, hbm = pl.BlockSpec(memory_space=pltpu.VMEM), pl.BlockSpec(memory_space=pltpu.HBM)
    dma = pltpu.SemaphoreType.DMA
    return pl.pallas_call(
        functools.partial(dispatch_kernel, dims),
        name="dispatch",
        out_shape=(jax.ShapeDtypeStruct((slots, width), BF16), jax.ShapeDtypeStruct(ids.shape, jnp.int32)),
        in_specs=[vmem, vmem, hbm],
        out_specs=(hbm, vmem),
        scratch_shapes=[
            pltpu.VMEM((rows, LANES), jnp.int32),
            pltpu.VMEM((rows, num_experts, 2 * LANES), F32),
            pltpu.VMEM((rows, LANES), jnp.int32),
            pltpu.VMEM((2 * slot_rows, rows * LANES), BF16),
            pltpu.VMEM((LANES, rows * LANES), BF16),
            pltpu.VMEM((slot_rows, LANES), jnp.int32),
            pltpu.SMEM((slot_rows, LANES), jnp.int32),
            pltpu.VMEM((tok_dev, width), BF16),
            pltpu.VMEM((tok_dev * parts + 8, LANES), F32),
            pltpu.VMEM((LANES * parts + 8, LANES), F32),
            pltpu.VMEM((slots, width), BF16),
            dma, dma, dma,
        ],
        compiler_params=pltpu.CompilerParams(vmem_limit_bytes=60 << 20),
        cost_estimate=pl.CostEstimate(flops=20_000_000_000, bytes_accessed=15_000_000, transcendentals=0),
    )(ids, order, tok_rows)


def pick(table, t):
    value = jnp.int32(0)
    for i, entry in enumerate(table):
        if entry:
            value = value + jnp.where(t == i, entry, 0)
    return value


def experts_kernel(dims, ids_ref, wr_ref, keys_ref, tau_ref, tok_hbm, send, w1_hbm, w2_hbm, b1_hbm, b2_hbm,
                   back_hbm, gate_ref, stage, recv, w1, w2, b1, b2,
                   tok_sem, wout_sem, win_sem, out_sem, in_sem, ret_sem, back_sem):
    size_b, size_x, cap = dims
    n = size_x
    rows = ids_ref.shape[0]
    num_experts = 2 * size_b * size_x
    tok_dev, chunk = tok_hbm.shape[0], stage.shape[1]
    i_dp, i_b, i_a = lax.axis_index("dp"), lax.axis_index("ep_b"), lax.axis_index("ep_a")
    pos_x, core, pos_y = i_a // 2, lax.rem(i_a, 2), i_b
    pos = (1 - core) * pos_x + core * pos_y
    wpos = (1 - core) * pos_y + core * pos_x

    def sends_to(kind, k):
        return i_dp, (1 - kind) * pos_y + kind * k, 2 * ((1 - kind) * k + kind * pos_x) + kind

    def serves(k, c):
        return i_dp, core * k + (1 - core) * pos_y, 2 * (core * pos_x + (1 - core) * k) + c

    def shares(k):
        return i_dp, (1 - core) * k + core * pos_y, 2 * ((1 - core) * pos_x + core * k) + core

    def block(i):
        return pl.ds(pl.multiple_of(i * cap, cap), cap)

    def fetch(q):
        return pltpu.make_async_copy(tok_hbm.at[pl.ds(pl.multiple_of(q * chunk, chunk), chunk)], stage.at[lax.rem(q, 2)],
                                     tok_sem.at[lax.rem(q, 2)])

    def each_chunk(body):
        chunks = tok_dev // chunk

        def step(q, _):
            @pl.when(q + 1 < chunks)
            def _():
                fetch(q + 1).start()
            fetch(q).wait()
            body(q, lax.rem(q, 2))
            return 0

        lax.fori_loop(0, chunks, step, 0)

    fetch(0).start()
    held = ((w1_hbm, w1), (w2_hbm, w2), (b1_hbm, b1), (b2_hbm, b2))
    for i, (own, every) in enumerate(held):
        pltpu.make_async_copy(own, every.at[pl.ds(0, 1)], win_sem.at[i, 0]).start()

    barrier = pltpu.get_barrier_semaphore()
    for k in range(n):
        for c in range(2):
            for device in (sends_to(c, k), serves(k, c)):
                pl.semaphore_signal(barrier, inc=1, device_id=device, device_id_type=MESH_ID)
    for d in range(1, n):
        pl.semaphore_signal(barrier, inc=1, device_id=shares(lax.rem(wpos + d, n)), device_id_type=MESH_ID)
    pl.semaphore_wait(barrier, 5 * n - 1)

    def weight_copy(i, d):
        own, every = held[i]
        return pltpu.make_async_remote_copy(
            src_ref=own, dst_ref=every.at[pl.ds(d, 1)], send_sem=wout_sem.at[i, d], recv_sem=win_sem.at[i, d],
            device_id=shares(lax.rem(wpos - d + n, n)), device_id_type=MESH_ID)

    weight_order = [1, n - 1] + list(range(2, n - 1))
    for d in weight_order:
        for i in (2, 3, 0, 1):
            weight_copy(i, d).start()

    iota_exp = iota((num_experts, LANES), 0)

    near, far = [1, n - 1], list(range(2, n - 1))
    send_order = [(step, off, kind) for group in (near, far, [0]) for off in range(n) for step in group for kind in range(2)]

    def outgoing(t):
        step, off, kind = (pick([e[i] for e in send_order], t) for i in range(3))
        k = lax.rem((1 - kind) * pos_x + kind * pos_y + step, n)
        j = lax.rem((1 - kind) * pos_y + kind * pos_x + off, n)
        return step, kind, k, j

    def send_block(t):
        step, kind, k, j = outgoing(t)
        src = (kind * n + k) * n + j
        dst = (((1 - kind) * pos_x + kind * pos_y) * n + j) * 2 + core
        own = (step == 0) & (kind == core)

        @pl.when(own)
        def _():
            pltpu.make_async_copy(send.at[block(src)], recv.at[block(dst)], in_sem.at[dst]).start()

        @pl.when(jnp.logical_not(own))
        def _():
            pltpu.make_async_remote_copy(
                src_ref=send.at[block(src)], dst_ref=recv.at[block(dst)], send_sem=out_sem.at[src], recv_sem=in_sem.at[dst],
                device_id=sends_to(kind, k), device_id_type=MESH_ID).start()

    blocks = 2 * n * n
    lax.fori_loop(0, blocks, lambda t, _: (send_block(t), 0)[1], 0)

    keys = keys_ref[...].astype(F32)
    key_unit = keys / jnp.sqrt(jnp.sum(keys * keys, axis=1, keepdims=True))
    tau = tau_ref[0, 0]
    key_pad = jnp.concatenate([key_unit, jnp.zeros((LANES - num_experts, key_unit.shape[1]), F32)], axis=0)
    span = chunk // LANES

    def gate_rows(i, slot):
        r = jnp.dot(stage[slot], wr_ref[...], preferred_element_type=F32)
        unit = r / jnp.sqrt(jnp.sum(r * r, axis=1, keepdims=True))
        dots = lax.dot_general(unit, key_pad, (((1,), (1,)), ((), ())), preferred_element_type=F32,
                               precision=lax.Precision.HIGHEST)
        logits = dots.T[:num_experts] / tau
        p = jnp.exp(logits - jnp.max(logits, axis=0, keepdims=True))
        total = jnp.sum(p, axis=0, keepdims=True)
        for q in range(span):
            mine = iota_exp == ids_ref[pl.ds(i * span + q, 1), :]
            cols = slice(q * LANES, (q + 1) * LANES)
            gate_ref[pl.ds(i * span + q, 1), :] = jnp.sum(jnp.where(mine, p[:, cols], 0.0), axis=0, keepdims=True) / total[:, cols]

    each_chunk(gate_rows)

    serve_order = ([(0, off) for off in range(n // 2)] + [(step, off) for off in range(n) for step in near]
                   + [(0, off) for off in range(n // 2, n - 1)] + [(step, off) for step in far for off in range(n)] + [(0, n - 1)])
    first_use = [int(off not in [o for _, o in serve_order[:i]]) for i, (_, off) in enumerate(serve_order)]

    def incoming(t):
        step, off = (pick([e[i] for e in serve_order], t) for i in range(2))
        return lax.rem(pos - step + n, n), off, lax.rem(wpos + off, n)

    def result_ends(t, c):
        k, _, j = incoming(t)
        src, dst = (k * n + j) * 2 + c, (core * n + pos) * n + j
        return k, src, dst, (k == pos) & (core == c)

    def send_results(t):
        for c in range(2):
            k, src, dst, own = result_ends(t, c)

            @pl.when(own)
            def _():
                pltpu.make_async_copy(recv.at[block(src)], back_hbm.at[block(dst)], back_sem.at[dst]).start()

            @pl.when(jnp.logical_not(own))
            def _():
                pltpu.make_async_remote_copy(
                    src_ref=recv.at[block(src)], dst_ref=back_hbm.at[block(dst)], send_sem=ret_sem.at[src],
                    recv_sem=back_sem.at[dst], device_id=serves(k, c), device_id_type=MESH_ID).start()

    def serve(t, _):
        k, off, j = incoming(t)
        first = (k * n + j) * 2

        @pl.when(pick(first_use, t) == 1)
        def _():
            for i, (own, every) in enumerate(held):
                pltpu.make_async_copy(own, every.at[pl.ds(off, 1)], win_sem.at[i, off]).wait()

        for c in range(2):
            pltpu.make_async_copy(send.at[block(0)], recv.at[block(first + c)], in_sem.at[first + c]).wait()
        here = pl.ds(pl.multiple_of(first * cap, 2 * cap), 2 * cap)
        hidden = jnp.dot(recv[here, :], w1[off], preferred_element_type=F32) + b1[off].astype(F32)
        hidden = (0.5 * hidden * (1.0 + lax.erf(hidden * (0.5 ** 0.5)))).astype(BF16)
        y = jnp.dot(hidden, w2[off], preferred_element_type=F32) + b2[off].astype(F32)
        recv[here, :] = y.astype(BF16)

        @pl.when(t > 0)
        def _():
            send_results(t - 1)
        return 0

    lax.fori_loop(0, n * n, serve, 0)
    send_results(jnp.int32(n * n - 1))

    for d in range(1, n):
        for i in range(len(held)):
            weight_copy(i, d).wait_send()

    def drain(t, _):
        sent = pltpu.make_async_remote_copy(
            src_ref=send.at[block(t)], dst_ref=recv.at[block(t)], send_sem=out_sem.at[t], recv_sem=in_sem.at[t],
            device_id=(i_dp, i_b, i_a), device_id_type=MESH_ID)
        returned = pltpu.make_async_remote_copy(
            src_ref=recv.at[block(t)], dst_ref=back_hbm.at[block(t)], send_sem=ret_sem.at[t], recv_sem=back_sem.at[t],
            device_id=(i_dp, i_b, i_a), device_id_type=MESH_ID)
        kind, k = t // (n * n), lax.rem(t // n, n)

        @pl.when((kind != core) | (k != pos))
        def _():
            sent.wait_send()

        @pl.when((t // (2 * n) != pos) | (lax.rem(t, 2) != core))
        def _():
            returned.wait_send()

        returned.wait_recv()
        return 0

    lax.fori_loop(0, blocks, drain, 0)


def experts(tok_rows, ids, send_rows, w_route, expert_keys, temperature, w1, w2, b1, b2, dims):
    size_b, size_x, cap = dims
    n = size_x
    tok_dev, width = tok_rows.shape
    hidden = w1.shape[2]
    slots = send_rows.shape[0]
    vmem, smem, hbm = (pl.BlockSpec(memory_space=m) for m in (pltpu.VMEM, pltpu.SMEM, pltpu.HBM))
    dma = pltpu.SemaphoreType.DMA
    return pl.pallas_call(
        functools.partial(experts_kernel, dims),
        name="experts",
        out_shape=(jax.ShapeDtypeStruct((slots, width), BF16), jax.ShapeDtypeStruct(ids.shape, F32)),
        in_specs=[vmem] * 3 + [smem] + [hbm] * 6,
        out_specs=(hbm, vmem),
        scratch_shapes=[
            pltpu.VMEM((2, min(tok_dev, 512), width), BF16),
            pltpu.VMEM((slots, width), BF16),
            pltpu.VMEM((n, width, hidden), BF16),
            pltpu.VMEM((n, hidden, width), BF16),
            pltpu.VMEM((n, 1, hidden), BF16),
            pltpu.VMEM((n, 1, width), BF16),
            dma((2,)), dma((4, n)), dma((4, n)),
            dma((2 * n * n,)), dma((2 * n * n,)), dma((2 * n * n,)), dma((2 * n * n,)),
        ],
        compiler_params=pltpu.CompilerParams(collective_id=1, has_side_effects=True, vmem_limit_bytes=61 << 20),
        cost_estimate=pl.CostEstimate(flops=4 * slots * width * hidden, bytes_accessed=30_000_000, transcendentals=0),
    )(ids, w_route, expert_keys, temperature.reshape(1, 1), tok_rows, send_rows, w1, w2, b1, b2)


def combine_kernel(back_hbm, dest_hbm, gate_ref, out_ref, stage, big, tmp, dest_sm, sem, dest_sem):
    i = pl.program_id(0)
    slots, width = back_hbm.shape
    parts = width // LANES
    chunk = stage.shape[1]
    chunks = slots // chunk

    @pl.when(i == 0)
    def _():
        def fetch(q):
            return pltpu.make_async_copy(back_hbm.at[pl.ds(pl.multiple_of(q * chunk, chunk), chunk)], stage.at[lax.rem(q, 2)],
                                         sem.at[lax.rem(q, 2)])
        fetch(0).start()
        dest_copy = pltpu.make_async_copy(dest_hbm, dest_sm, dest_sem)
        dest_copy.start()
        big[pl.ds(slots * parts, 8), :] = jnp.zeros((8, LANES), F32)

        def widen_chunk(q, _):
            @pl.when(q + 1 < chunks)
            def _():
                fetch(q + 1).start()
            fetch(q).wait()

            def widen(u, _):
                base = pl.multiple_of(u * 16, 16)
                for c in range(parts):
                    big[pl.ds((q * chunk + base) * parts + c, 16, stride=parts), :] = (
                        stage[lax.rem(q, 2), pl.ds(base, 16), c * LANES:(c + 1) * LANES].astype(F32))
                return 0

            lax.fori_loop(0, chunk // 16, widen, 0, unroll=8)
            return 0

        lax.fori_loop(0, chunks, widen_chunk, 0)
        dest_copy.wait()

    def gather(g, _):
        row = i * (out_ref.shape[0] // LANES) + g
        for j in range(LANES):
            tmp[pl.ds(j * parts, parts), :] = big[pl.ds(dest_sm[row, j], parts), :]
        gate = jnp.broadcast_to(gate_ref[pl.ds(row, 1), :], (LANES, LANES)).T
        for j in range(0, LANES, 16):
            for c in range(parts):
                out_ref[pl.ds(pl.multiple_of(g * LANES + j, 16), 16), c * LANES:(c + 1) * LANES] = (
                    (gate[j:j + 16] * tmp[pl.ds(j * parts + c, 16, stride=parts), :]).astype(BF16))
        return 0

    lax.fori_loop(0, out_ref.shape[0] // LANES, gather, 0)


def combine(back_rows, dest, gate, tok_dev):
    slots, width = back_rows.shape
    parts = width // LANES
    block = 1024
    hbm = pl.BlockSpec(memory_space=pltpu.HBM)
    return pl.pallas_call(
        combine_kernel,
        name="combine",
        grid=(tok_dev // block,),
        out_shape=jax.ShapeDtypeStruct((tok_dev, width), BF16),
        in_specs=[hbm, hbm, pl.BlockSpec(memory_space=pltpu.VMEM)],
        out_specs=pl.BlockSpec((block, width), lambda i: (i, 0)),
        scratch_shapes=[
            pltpu.VMEM((2, 1280, width), BF16),
            pltpu.VMEM((slots * parts + 8, LANES), F32),
            pltpu.VMEM((LANES * parts + 8, LANES), F32),
            pltpu.SMEM(dest.shape, jnp.int32),
            pltpu.SemaphoreType.DMA((2,)),
            pltpu.SemaphoreType.DMA,
        ],
        compiler_params=pltpu.CompilerParams(vmem_limit_bytes=40 << 20, dimension_semantics=("arbitrary",)),
        cost_estimate=pl.CostEstimate(flops=20_000_000_000, bytes_accessed=15_000_000, transcendentals=0),
    )(back_rows, dest, gate)


def solution(mesh):
    size_b, size_x = mesh.shape["ep_b"], mesh.shape["ep_a"] // 2
    num_experts = 2 * size_b * size_x
    tok_spec = P(("dp",) + EXPERT_AXES)
    expert_spec = P(EXPERT_AXES)

    def device_step(tokens, expert_ids, route_order, w_route, expert_keys, temperature, w_in, b_in, w_out, b_out):
        tok_dev = tokens.shape[1]
        cap = (5 * tok_dev + 4 * num_experts - 1) // (4 * num_experts)
        dims = (size_b, size_x, cap)
        ids = expert_ids.reshape(tok_dev // LANES, LANES)
        send_rows, dest = dispatch(tokens[0], ids, route_order.reshape(ids.shape), dims)
        back_rows, gate = experts(tokens[0], ids, send_rows, w_route, expert_keys, temperature, w_in, w_out,
                                  b_in[:, None, :], b_out[:, None, :], dims)
        return combine(back_rows, dest, gate, tok_dev)[None]

    return jax.shard_map(
        device_step,
        mesh=mesh,
        in_specs=(tok_spec, tok_spec, tok_spec, P(), P(), P(), expert_spec, expert_spec, expert_spec, expert_spec),
        out_specs=tok_spec,
        check_vma=False,
    )
```

```python
import functools

import jax
import jax.numpy as jnp
from jax import lax
from jax.experimental import pallas as pl
from jax.experimental.pallas import tpu as pltpu
from jax.sharding import PartitionSpec as P

EXPERT_AXES = ("ep_b", "ep_a")
LANES = 128
MESH_ID = pl.DeviceIdType.MESH
F32 = jnp.float32
BF16 = jnp.bfloat16


def iota(shape, dim):
    return lax.broadcasted_iota(jnp.int32, shape, dim)


def dot_nt(a, b):
    return lax.dot_general(a, b, (((1,), (1,)), ((), ())), preferred_element_type=F32)


def as_bf16(mask):
    return jnp.where(mask, 1.0, 0.0).astype(BF16)


def virtual_expert(ids, size_b, size_x):
    i_b, i_a = ids // (2 * size_x), ids % (2 * size_x)
    x, core = i_a // 2, i_a % 2
    return jnp.where(core == 0, x * size_b + i_b, size_b * size_x + i_b * size_x + x)


def dispatch_kernel(dims, ids_ref, order_ref, tok_hbm, send_hbm, dest_ref,
                    rid_s, both_s, kept_s, hi_s, lo_s, src_vm, src_sm, tok_vm, big, tmp, send, tok_sem, src_sem, out_sem):
    size_b, size_x, cap = dims
    rows, slot_rows = ids_ref.shape[0], src_vm.shape[0]
    parts = tok_hbm.shape[1] // LANES
    tok_copy = pltpu.make_async_copy(tok_hbm, tok_vm, tok_sem)
    tok_copy.start()
    num_experts = 2 * size_b * size_x
    per_expert = slot_rows // num_experts
    upper = as_bf16((iota((LANES, 2 * LANES), 0) <= iota((LANES, 2 * LANES), 1)) | (iota((LANES, 2 * LANES), 1) >= LANES))
    ids_t = ids_ref[...].astype(F32).T.astype(BF16)
    iota_rows = iota((rows, LANES), 0)
    iota_lane = iota((LANES, LANES), 0)
    iota_exp = iota((num_experts, LANES), 0)
    iota_slot = iota((slot_rows, LANES), 0)
    zero_count = jnp.zeros((num_experts, LANES), F32)

    def row(r):
        return pl.ds(r, 1)

    def cols(r):
        return pl.ds(pl.multiple_of(r * LANES, LANES), LANES)

    def each(body, unroll):
        lax.fori_loop(0, rows, lambda r, _: (body(r), 0)[1], 0, unroll=unroll)

    def ranked_id(r):
        o = order_ref[row(r), :]
        table = jnp.dot(ids_t, as_bf16(iota_rows == o // LANES), preferred_element_type=F32)
        rid_s[row(r), :] = jnp.sum(jnp.where(iota_lane == o % LANES, table, 0.0), axis=0, keepdims=True).astype(jnp.int32)

    def ranked_count(r):
        both_s[r] = jnp.dot(as_bf16(iota_exp == rid_s[row(r), :]), upper, preferred_element_type=F32)

    def position(mine, r, count):
        return jnp.sum(jnp.where(mine, both_s[r, :, :LANES] + count, 0.0), axis=0, keepdims=True)

    def ranked_kept(r, count):
        rank = position(iota_exp == rid_s[row(r), :], r, count)
        kept_s[row(r), :] = (rank <= float(cap)).astype(jnp.int32)
        return count + both_s[r, :, LANES:]

    def scatter_kept(r):
        o = order_ref[row(r), :]
        hi_s[:rows, cols(r)] = as_bf16((iota_rows == o // LANES) & (kept_s[row(r), :] > 0))
        lo_s[:, cols(r)] = as_bf16(iota_lane == o % LANES)

    each(ranked_id, 16)
    each(ranked_count, 16)
    lax.fori_loop(0, rows, ranked_kept, zero_count, unroll=8)
    each(scatter_kept, 8)
    kept_s[...] = dot_nt(hi_s[:rows, :], lo_s[...]).astype(jnp.int32)

    def expert_of(r):
        return virtual_expert(ids_ref[row(r), :], size_b, size_x)

    def mine_kept(r):
        return (iota_exp == expert_of(r)) & (kept_s[row(r), :] > 0)

    def token_count(r):
        both_s[r] = jnp.dot(as_bf16(mine_kept(r)), upper, preferred_element_type=F32)

    lane = iota((1, LANES), 1).astype(F32)

    def placed(r, count):
        place = position(mine_kept(r), r, count).astype(jnp.int32) - 1
        kept = kept_s[row(r), :] > 0
        expert = expert_of(r)
        dest_ref[row(r), :] = jnp.where(kept, expert * cap + place, num_experts * cap) * parts
        rid_s[row(r), :] = jnp.where(kept, expert * (per_expert * LANES) + place, slot_rows * LANES)
        return count + both_s[r, :, LANES:]

    def scatter_source(r):
        slot = rid_s[row(r), :]
        hit = jnp.where(iota_slot == slot // LANES, 1.0, 0.0)
        hi_s[:slot_rows, cols(r)] = (hit * lax.convert_element_type(r, F32)).astype(BF16)
        hi_s[slot_rows:, cols(r)] = (hit * lane).astype(BF16)
        lo_s[:, cols(r)] = as_bf16(iota_lane == slot % LANES)

    each(token_count, 16)
    lax.fori_loop(0, rows, placed, zero_count, unroll=8)
    each(scatter_source, 8)
    found = dot_nt(hi_s[...], lo_s[...])
    src_vm[...] = ((found[:slot_rows] * float(LANES) + found[slot_rows:]) * float(parts)).astype(jnp.int32)
    src_copy = pltpu.make_async_copy(src_vm, src_sm, src_sem)
    src_copy.start()

    tok_copy.wait()

    def widen(i, _):
        base = pl.multiple_of(i * 16, 16)
        for c in range(parts):
            big[pl.ds(base * parts + c, 16, stride=parts), :] = tok_vm[pl.ds(base, 16), c * LANES:(c + 1) * LANES].astype(F32)
        return 0

    lax.fori_loop(0, tok_vm.shape[0] // 16, widen, 0, unroll=8)
    src_copy.wait()

    def gather_rows(row_index, first, count):
        for u in range(count):
            tmp[pl.ds(u * parts, parts), :] = big[pl.ds(src_sm[row_index, u], parts), :]
        for u in range(0, count, 16):
            for c in range(parts):
                send[pl.ds(pl.multiple_of(first + u, 16), 16), c * LANES:(c + 1) * LANES] = (
                    tmp[pl.ds(u * parts + c, 16, stride=parts), :].astype(BF16))

    def out_copy(index):
        rows_of = pl.ds(pl.multiple_of(index * cap, cap), cap)
        return pltpu.make_async_copy(send.at[rows_of], send_hbm.at[rows_of], out_sem)

    def gather_block(index, _):
        def gather(g, _):
            gather_rows(index * per_expert + g, pl.multiple_of(index * cap + g * LANES, 16), LANES)
            return 0

        lax.fori_loop(0, cap // LANES, gather, 0)
        if cap % LANES:
            gather_rows(index * per_expert + cap // LANES, pl.multiple_of(index * cap + cap // LANES * LANES, 16), cap % LANES)
        out_copy(index).start()
        return 0

    lax.fori_loop(0, num_experts, gather_block, 0)
    lax.fori_loop(0, num_experts, lambda index, _: (out_copy(index).wait(), 0)[1], 0)


def dispatch(tok_rows, ids, order, dims):
    size_b, size_x, cap = dims
    num_experts = 2 * size_b * size_x
    slots, slot_rows = num_experts * cap, num_experts * pl.cdiv(cap, LANES)
    tok_dev, width = tok_rows.shape
    rows, parts = tok_dev // LANES, width // LANES
    vmem, hbm = pl.BlockSpec(memory_space=pltpu.VMEM), pl.BlockSpec(memory_space=pltpu.HBM)
    dma = pltpu.SemaphoreType.DMA
    return pl.pallas_call(
        functools.partial(dispatch_kernel, dims),
        name="dispatch",
        out_shape=(jax.ShapeDtypeStruct((slots, width), BF16), jax.ShapeDtypeStruct(ids.shape, jnp.int32)),
        in_specs=[vmem, vmem, hbm],
        out_specs=(hbm, vmem),
        scratch_shapes=[
            pltpu.VMEM((rows, LANES), jnp.int32),
            pltpu.VMEM((rows, num_experts, 2 * LANES), F32),
            pltpu.VMEM((rows, LANES), jnp.int32),
            pltpu.VMEM((2 * slot_rows, rows * LANES), BF16),
            pltpu.VMEM((LANES, rows * LANES), BF16),
            pltpu.VMEM((slot_rows, LANES), jnp.int32),
            pltpu.SMEM((slot_rows, LANES), jnp.int32),
            pltpu.VMEM((tok_dev, width), BF16),
            pltpu.VMEM((tok_dev * parts + 8, LANES), F32),
            pltpu.VMEM((LANES * parts + 8, LANES), F32),
            pltpu.VMEM((slots, width), BF16),
            dma, dma, dma,
        ],
        compiler_params=pltpu.CompilerParams(vmem_limit_bytes=60 << 20),
        cost_estimate=pl.CostEstimate(flops=20_000_000_000, bytes_accessed=15_000_000, transcendentals=0),
    )(ids, order, tok_rows)


def pick(table, t):
    value = jnp.int32(0)
    for i, entry in enumerate(table):
        if entry:
            value = value + jnp.where(t == i, entry, 0)
    return value


def experts_kernel(dims, ids_ref, wr_ref, keys_ref, tau_ref, tok_hbm, send, w1_hbm, w2_hbm, b1_hbm, b2_hbm,
                   back_hbm, gate_ref, stage, recv, w1, w2, b1, b2,
                   tok_sem, wout_sem, win_sem, out_sem, in_sem, ret_sem, back_sem):
    size_b, size_x, cap = dims
    n = size_x
    rows = ids_ref.shape[0]
    num_experts = 2 * size_b * size_x
    tok_dev, chunk = tok_hbm.shape[0], stage.shape[1]
    i_dp, i_b, i_a = lax.axis_index("dp"), lax.axis_index("ep_b"), lax.axis_index("ep_a")
    pos_x, core, pos_y = i_a // 2, lax.rem(i_a, 2), i_b
    pos = (1 - core) * pos_x + core * pos_y
    wpos = (1 - core) * pos_y + core * pos_x

    def sends_to(kind, k):
        return i_dp, (1 - kind) * pos_y + kind * k, 2 * ((1 - kind) * k + kind * pos_x) + kind

    def serves(k, c):
        return i_dp, core * k + (1 - core) * pos_y, 2 * (core * pos_x + (1 - core) * k) + c

    def shares(k):
        return i_dp, (1 - core) * k + core * pos_y, 2 * ((1 - core) * pos_x + core * k) + core

    def block(i):
        return pl.ds(pl.multiple_of(i * cap, cap), cap)

    def fetch(q):
        return pltpu.make_async_copy(tok_hbm.at[pl.ds(pl.multiple_of(q * chunk, chunk), chunk)], stage.at[lax.rem(q, 2)],
                                     tok_sem.at[lax.rem(q, 2)])

    def each_chunk(body):
        chunks = tok_dev // chunk

        def step(q, _):
            @pl.when(q + 1 < chunks)
            def _():
                fetch(q + 1).start()
            fetch(q).wait()
            body(q, lax.rem(q, 2))
            return 0

        lax.fori_loop(0, chunks, step, 0)

    fetch(0).start()
    held = ((w1_hbm, w1), (w2_hbm, w2), (b1_hbm, b1), (b2_hbm, b2))
    for i, (own, every) in enumerate(held):
        pltpu.make_async_copy(own, every.at[pl.ds(0, 1)], win_sem.at[i, 0]).start()

    barrier = pltpu.get_barrier_semaphore()
    for k in range(n):
        for c in range(2):
            for device in (sends_to(c, k), serves(k, c)):
                pl.semaphore_signal(barrier, inc=1, device_id=device, device_id_type=MESH_ID)
    for d in range(1, n):
        pl.semaphore_signal(barrier, inc=1, device_id=shares(lax.rem(wpos + d, n)), device_id_type=MESH_ID)
    pl.semaphore_wait(barrier, 5 * n - 1)

    def weight_copy(i, d):
        own, every = held[i]
        return pltpu.make_async_remote_copy(
            src_ref=own, dst_ref=every.at[pl.ds(d, 1)], send_sem=wout_sem.at[i, d], recv_sem=win_sem.at[i, d],
            device_id=shares(lax.rem(wpos - d + n, n)), device_id_type=MESH_ID)

    near, far = [1, n - 1], list(range(2, n - 1))
    for d in near + far:
        for i in (2, 3):
            weight_copy(i, d).start()
    for first, d in enumerate(near):
        for i in (first, 1 - first):
            weight_copy(i, d).start()

    def passed_on(i):
        every = held[i][1]
        d, to = near[i], (wpos - 1 + n, wpos + 1)[i]
        return pltpu.make_async_remote_copy(
            src_ref=every.at[pl.ds(d, 1)], dst_ref=every.at[pl.ds(2, 1)], send_sem=wout_sem.at[i, 2], recv_sem=win_sem.at[i, 2],
            device_id=shares(lax.rem(to, n)), device_id_type=MESH_ID)

    def weights_here(i, off):
        own, every = held[i]
        pltpu.make_async_copy(own, every.at[pl.ds(off, 1)], win_sem.at[i, off]).wait()

    iota_exp = iota((num_experts, LANES), 0)

    soon = [0] + near
    send_order = [(step, off, kind) for offs, group in ((soon, near), (soon, far), (soon, [0]), (far, near + far + [0]))
                  for off in offs for step in group for kind in range(2)]

    def outgoing(t):
        step, off, kind = (pick([e[i] for e in send_order], t) for i in range(3))
        k = lax.rem((1 - kind) * pos_x + kind * pos_y + step, n)
        j = lax.rem((1 - kind) * pos_y + kind * pos_x + off, n)
        return step, kind, k, j

    def send_block(t):
        step, kind, k, j = outgoing(t)
        src = (kind * n + k) * n + j
        dst = (((1 - kind) * pos_x + kind * pos_y) * n + j) * 2 + core
        own = (step == 0) & (kind == core)

        @pl.when(own)
        def _():
            pltpu.make_async_copy(send.at[block(src)], recv.at[block(dst)], in_sem.at[dst]).start()

        @pl.when(jnp.logical_not(own))
        def _():
            pltpu.make_async_remote_copy(
                src_ref=send.at[block(src)], dst_ref=recv.at[block(dst)], send_sem=out_sem.at[src], recv_sem=in_sem.at[dst],
                device_id=sends_to(kind, k), device_id_type=MESH_ID).start()

    blocks = 2 * n * n
    early = 2 * len(near)
    lax.fori_loop(0, early, lambda t, _: (send_block(t), 0)[1], 0)

    keys = keys_ref[...].astype(F32)
    key_unit = keys / jnp.sqrt(jnp.sum(keys * keys, axis=1, keepdims=True))
    tau = tau_ref[0, 0]
    key_pad = jnp.concatenate([key_unit, jnp.zeros((LANES - num_experts, key_unit.shape[1]), F32)], axis=0)
    span = chunk // LANES

    def gate_rows(i, slot):
        r = jnp.dot(stage[slot], wr_ref[...], preferred_element_type=F32)
        unit = r / jnp.sqrt(jnp.sum(r * r, axis=1, keepdims=True))
        dots = lax.dot_general(unit, key_pad, (((1,), (1,)), ((), ())), preferred_element_type=F32,
                               precision=lax.Precision.HIGHEST)
        logits = dots.T[:num_experts] / tau
        p = jnp.exp(logits - jnp.max(logits, axis=0, keepdims=True))
        total = jnp.sum(p, axis=0, keepdims=True)
        for q in range(span):
            mine = iota_exp == ids_ref[pl.ds(i * span + q, 1), :]
            cols = slice(q * LANES, (q + 1) * LANES)
            gate_ref[pl.ds(i * span + q, 1), :] = jnp.sum(jnp.where(mine, p[:, cols], 0.0), axis=0, keepdims=True) / total[:, cols]

    each_chunk(gate_rows)

    for i in range(2):
        weights_here(i, near[i])
        passed_on(i).start()
    lax.fori_loop(early, blocks, lambda t, _: (send_block(t), 0)[1], 0)

    serve_order = ([(0, off) for off in soon] + [(step, off) for off in soon for step in near]
                   + [(step, off) for step in far for off in soon] + [(step, off) for off in far for step in near + far + [0]])
    first_use = [[int(off not in [o for _, o in serve_order[:t]] and (i > 1 or off != near[i]))
                  for t, (_, off) in enumerate(serve_order)] for i in range(len(held))]

    def incoming(t):
        step, off = (pick([e[i] for e in serve_order], t) for i in range(2))
        return lax.rem(pos - step + n, n), off, lax.rem(wpos + off, n)

    def result_ends(t, c):
        k, _, j = incoming(t)
        src, dst = (k * n + j) * 2 + c, (core * n + pos) * n + j
        return k, src, dst, (k == pos) & (core == c)

    def send_results(t):
        for c in range(2):
            k, src, dst, own = result_ends(t, c)

            @pl.when(own)
            def _():
                pltpu.make_async_copy(recv.at[block(src)], back_hbm.at[block(dst)], back_sem.at[dst]).start()

            @pl.when(jnp.logical_not(own))
            def _():
                pltpu.make_async_remote_copy(
                    src_ref=recv.at[block(src)], dst_ref=back_hbm.at[block(dst)], send_sem=ret_sem.at[src],
                    recv_sem=back_sem.at[dst], device_id=serves(k, c), device_id_type=MESH_ID).start()

    def serve(t, _):
        k, off, j = incoming(t)
        first = (k * n + j) * 2

        for i in range(len(held)):
            @pl.when(pick(first_use[i], t) == 1)
            def _():
                weights_here(i, off)

        for c in range(2):
            pltpu.make_async_copy(send.at[block(0)], recv.at[block(first + c)], in_sem.at[first + c]).wait()
        here = pl.ds(pl.multiple_of(first * cap, 2 * cap), 2 * cap)
        hidden = jnp.dot(recv[here, :], w1[off], preferred_element_type=F32) + b1[off].astype(F32)
        hidden = (0.5 * hidden * (1.0 + lax.erf(hidden * (0.5 ** 0.5)))).astype(BF16)
        y = jnp.dot(hidden, w2[off], preferred_element_type=F32) + b2[off].astype(F32)
        recv[here, :] = y.astype(BF16)

        @pl.when(t > 0)
        def _():
            send_results(t - 1)
        return 0

    lax.fori_loop(0, n * n, serve, 0)
    send_results(jnp.int32(n * n - 1))

    for d in near + far:
        for i in range(len(held)):
            (passed_on(i) if d == 2 and i < 2 else weight_copy(i, d)).wait_send()

    def drain(t, _):
        sent = pltpu.make_async_remote_copy(
            src_ref=send.at[block(t)], dst_ref=recv.at[block(t)], send_sem=out_sem.at[t], recv_sem=in_sem.at[t],
            device_id=(i_dp, i_b, i_a), device_id_type=MESH_ID)
        returned = pltpu.make_async_remote_copy(
            src_ref=recv.at[block(t)], dst_ref=back_hbm.at[block(t)], send_sem=ret_sem.at[t], recv_sem=back_sem.at[t],
            device_id=(i_dp, i_b, i_a), device_id_type=MESH_ID)
        kind, k = t // (n * n), lax.rem(t // n, n)

        @pl.when((kind != core) | (k != pos))
        def _():
            sent.wait_send()

        @pl.when((t // (2 * n) != pos) | (lax.rem(t, 2) != core))
        def _():
            returned.wait_send()

        returned.wait_recv()
        return 0

    lax.fori_loop(0, blocks, drain, 0)


def experts(tok_rows, ids, send_rows, w_route, expert_keys, temperature, w1, w2, b1, b2, dims):
    size_b, size_x, cap = dims
    n = size_x
    tok_dev, width = tok_rows.shape
    hidden = w1.shape[2]
    slots = send_rows.shape[0]
    vmem, smem, hbm = (pl.BlockSpec(memory_space=m) for m in (pltpu.VMEM, pltpu.SMEM, pltpu.HBM))
    dma = pltpu.SemaphoreType.DMA
    return pl.pallas_call(
        functools.partial(experts_kernel, dims),
        name="experts",
        out_shape=(jax.ShapeDtypeStruct((slots, width), BF16), jax.ShapeDtypeStruct(ids.shape, F32)),
        in_specs=[vmem] * 3 + [smem] + [hbm] * 6,
        out_specs=(hbm, vmem),
        scratch_shapes=[
            pltpu.VMEM((2, min(tok_dev, 512), width), BF16),
            pltpu.VMEM((slots, width), BF16),
            pltpu.VMEM((n, width, hidden), BF16),
            pltpu.VMEM((n, hidden, width), BF16),
            pltpu.VMEM((n, 1, hidden), BF16),
            pltpu.VMEM((n, 1, width), BF16),
            dma((2,)), dma((4, n)), dma((4, n)),
            dma((2 * n * n,)), dma((2 * n * n,)), dma((2 * n * n,)), dma((2 * n * n,)),
        ],
        compiler_params=pltpu.CompilerParams(collective_id=1, has_side_effects=True, vmem_limit_bytes=61 << 20),
        cost_estimate=pl.CostEstimate(flops=4 * slots * width * hidden, bytes_accessed=30_000_000, transcendentals=0),
    )(ids, w_route, expert_keys, temperature.reshape(1, 1), tok_rows, send_rows, w1, w2, b1, b2)


def combine_kernel(back_hbm, dest_ref, gate_ref, out_ref, stage, big, tmp, dest_sm, sem, dest_sem):
    i = pl.program_id(0)
    slots, width = back_hbm.shape
    parts = width // LANES
    chunk = stage.shape[1]
    chunks = slots // chunk

    @pl.when(i == 0)
    def _():
        def fetch(q):
            return pltpu.make_async_copy(back_hbm.at[pl.ds(pl.multiple_of(q * chunk, chunk), chunk)], stage.at[lax.rem(q, 2)],
                                         sem.at[lax.rem(q, 2)])
        fetch(0).start()
        dest_copy = pltpu.make_async_copy(dest_ref, dest_sm, dest_sem)
        dest_copy.start()
        big[pl.ds(slots * parts, 8), :] = jnp.zeros((8, LANES), F32)

        def widen_chunk(q, _):
            @pl.when(q + 1 < chunks)
            def _():
                fetch(q + 1).start()
            fetch(q).wait()

            def widen(u, _):
                base = pl.multiple_of(u * 16, 16)
                for c in range(parts):
                    big[pl.ds((q * chunk + base) * parts + c, 16, stride=parts), :] = (
                        stage[lax.rem(q, 2), pl.ds(base, 16), c * LANES:(c + 1) * LANES].astype(F32))
                return 0

            lax.fori_loop(0, chunk // 16, widen, 0, unroll=8)
            return 0

        lax.fori_loop(0, chunks, widen_chunk, 0)
        dest_copy.wait()

    def gather(g, _):
        row = i * (out_ref.shape[0] // LANES) + g
        for j in range(LANES):
            tmp[pl.ds(j * parts, parts), :] = big[pl.ds(dest_sm[row, j], parts), :]
        gate = jnp.broadcast_to(gate_ref[pl.ds(row, 1), :], (LANES, LANES)).T
        for j in range(0, LANES, 16):
            for c in range(parts):
                out_ref[pl.ds(pl.multiple_of(g * LANES + j, 16), 16), c * LANES:(c + 1) * LANES] = (
                    (gate[j:j + 16] * tmp[pl.ds(j * parts + c, 16, stride=parts), :]).astype(BF16))
        return 0

    lax.fori_loop(0, out_ref.shape[0] // LANES, gather, 0)


def combine(back_rows, dest, gate, tok_dev):
    slots, width = back_rows.shape
    parts = width // LANES
    block = 1024
    hbm = pl.BlockSpec(memory_space=pltpu.HBM)
    return pl.pallas_call(
        combine_kernel,
        name="combine",
        grid=(tok_dev // block,),
        out_shape=jax.ShapeDtypeStruct((tok_dev, width), BF16),
        in_specs=[hbm] + [pl.BlockSpec(memory_space=pltpu.VMEM)] * 2,
        out_specs=pl.BlockSpec((block, width), lambda i: (i, 0)),
        scratch_shapes=[
            pltpu.VMEM((2, 1280, width), BF16),
            pltpu.VMEM((slots * parts + 8, LANES), F32),
            pltpu.VMEM((LANES * parts + 8, LANES), F32),
            pltpu.SMEM(dest.shape, jnp.int32),
            pltpu.SemaphoreType.DMA((2,)),
            pltpu.SemaphoreType.DMA,
        ],
        compiler_params=pltpu.CompilerParams(vmem_limit_bytes=40 << 20, dimension_semantics=("arbitrary",)),
        cost_estimate=pl.CostEstimate(flops=20_000_000_000, bytes_accessed=15_000_000, transcendentals=0),
    )(back_rows, dest, gate)


def solution(mesh):
    size_b, size_x = mesh.shape["ep_b"], mesh.shape["ep_a"] // 2
    num_experts = 2 * size_b * size_x
    tok_spec = P(("dp",) + EXPERT_AXES)
    expert_spec = P(EXPERT_AXES)

    def device_step(tokens, expert_ids, route_order, w_route, expert_keys, temperature, w_in, b_in, w_out, b_out):
        tok_dev = tokens.shape[1]
        cap = (5 * tok_dev + 4 * num_experts - 1) // (4 * num_experts)
        dims = (size_b, size_x, cap)
        ids = expert_ids.reshape(tok_dev // LANES, LANES)
        send_rows, dest = dispatch(tokens[0], ids, route_order.reshape(ids.shape), dims)
        back_rows, gate = experts(tokens[0], ids, send_rows, w_route, expert_keys, temperature, w_in, w_out,
                                  b_in[:, None, :], b_out[:, None, :], dims)
        return combine(back_rows, dest, gate, tok_dev)[None]

    return jax.shard_map(
        device_step,
        mesh=mesh,
        in_specs=(tok_spec, tok_spec, tok_spec, P(), P(), P(), expert_spec, expert_spec, expert_spec, expert_spec),
        out_specs=tok_spec,
        check_vma=False,
    )
```

```python
import functools

import jax
import jax.numpy as jnp
from jax import lax
from jax.experimental import pallas as pl
from jax.experimental.pallas import tpu as pltpu
from jax.sharding import PartitionSpec as P

EXPERT_AXES = ("ep_b", "ep_a")
LANES = 128
MESH_ID = pl.DeviceIdType.MESH
F32 = jnp.float32
BF16 = jnp.bfloat16


def iota(shape, dim):
    return lax.broadcasted_iota(jnp.int32, shape, dim)


def dot_nt(a, b):
    return lax.dot_general(a, b, (((1,), (1,)), ((), ())), preferred_element_type=F32)


def as_bf16(mask):
    return jnp.where(mask, 1.0, 0.0).astype(BF16)


def virtual_expert(ids, size_b, size_x):
    i_b, i_a = ids // (2 * size_x), ids % (2 * size_x)
    x, core = i_a // 2, i_a % 2
    return jnp.where(core == 0, x * size_b + i_b, size_b * size_x + i_b * size_x + x)


def dispatch_kernel(dims, ids_ref, order_ref, tok_hbm, send_hbm, dest_ref,
                    rid_s, both_s, kept_s, hi_s, lo_s, src_vm, src_sm, tok_vm, big, tmp, send, tok_sem, src_sem, out_sem):
    size_b, size_x, cap = dims
    rows, slot_rows = ids_ref.shape[0], src_vm.shape[0]
    parts = tok_hbm.shape[1] // LANES
    tok_copy = pltpu.make_async_copy(tok_hbm, tok_vm, tok_sem)
    tok_copy.start()
    num_experts = 2 * size_b * size_x
    per_expert = slot_rows // num_experts
    upper = as_bf16((iota((LANES, 2 * LANES), 0) <= iota((LANES, 2 * LANES), 1)) | (iota((LANES, 2 * LANES), 1) >= LANES))
    ids_t = ids_ref[...].astype(F32).T.astype(BF16)
    iota_rows = iota((rows, LANES), 0)
    iota_lane = iota((LANES, LANES), 0)
    iota_exp = iota((num_experts, LANES), 0)
    iota_slot = iota((slot_rows, LANES), 0)
    zero_count = jnp.zeros((num_experts, LANES), F32)

    def row(r):
        return pl.ds(r, 1)

    def cols(r):
        return pl.ds(pl.multiple_of(r * LANES, LANES), LANES)

    def each(body, unroll):
        lax.fori_loop(0, rows, lambda r, _: (body(r), 0)[1], 0, unroll=unroll)

    def ranked_id(r):
        o = order_ref[row(r), :]
        table = jnp.dot(ids_t, as_bf16(iota_rows == o // LANES), preferred_element_type=F32)
        rid_s[row(r), :] = jnp.sum(jnp.where(iota_lane == o % LANES, table, 0.0), axis=0, keepdims=True).astype(jnp.int32)

    def ranked_count(r):
        both_s[r] = jnp.dot(as_bf16(iota_exp == rid_s[row(r), :]), upper, preferred_element_type=F32)

    def position(mine, r, count):
        return jnp.sum(jnp.where(mine, both_s[r, :, :LANES] + count, 0.0), axis=0, keepdims=True)

    def ranked_kept(r, count):
        rank = position(iota_exp == rid_s[row(r), :], r, count)
        kept_s[row(r), :] = (rank <= float(cap)).astype(jnp.int32)
        return count + both_s[r, :, LANES:]

    def scatter_kept(r):
        o = order_ref[row(r), :]
        hi_s[:rows, cols(r)] = as_bf16((iota_rows == o // LANES) & (kept_s[row(r), :] > 0))
        lo_s[:, cols(r)] = as_bf16(iota_lane == o % LANES)

    each(ranked_id, 16)
    each(ranked_count, 16)
    lax.fori_loop(0, rows, ranked_kept, zero_count, unroll=8)
    each(scatter_kept, 8)
    kept_s[...] = dot_nt(hi_s[:rows, :], lo_s[...]).astype(jnp.int32)

    def expert_of(r):
        return virtual_expert(ids_ref[row(r), :], size_b, size_x)

    def mine_kept(r):
        return (iota_exp == expert_of(r)) & (kept_s[row(r), :] > 0)

    def token_count(r):
        both_s[r] = jnp.dot(as_bf16(mine_kept(r)), upper, preferred_element_type=F32)

    lane = iota((1, LANES), 1).astype(F32)

    def placed(r, count):
        place = position(mine_kept(r), r, count).astype(jnp.int32) - 1
        kept = kept_s[row(r), :] > 0
        expert = expert_of(r)
        dest_ref[row(r), :] = jnp.where(kept, expert * cap + place, num_experts * cap) * parts
        rid_s[row(r), :] = jnp.where(kept, expert * (per_expert * LANES) + place, slot_rows * LANES)
        return count + both_s[r, :, LANES:]

    def scatter_source(r):
        slot = rid_s[row(r), :]
        hit = jnp.where(iota_slot == slot // LANES, 1.0, 0.0)
        hi_s[:slot_rows, cols(r)] = (hit * lax.convert_element_type(r, F32)).astype(BF16)
        hi_s[slot_rows:, cols(r)] = (hit * lane).astype(BF16)
        lo_s[:, cols(r)] = as_bf16(iota_lane == slot % LANES)

    each(token_count, 16)
    lax.fori_loop(0, rows, placed, zero_count, unroll=8)
    each(scatter_source, 8)
    found = dot_nt(hi_s[...], lo_s[...])
    src_vm[...] = ((found[:slot_rows] * float(LANES) + found[slot_rows:]) * float(parts)).astype(jnp.int32)
    src_copy = pltpu.make_async_copy(src_vm, src_sm, src_sem)
    src_copy.start()

    tok_copy.wait()

    def widen(i, _):
        base = pl.multiple_of(i * 16, 16)
        for c in range(parts):
            big[pl.ds(base * parts + c, 16, stride=parts), :] = tok_vm[pl.ds(base, 16), c * LANES:(c + 1) * LANES].astype(F32)
        return 0

    lax.fori_loop(0, tok_vm.shape[0] // 16, widen, 0, unroll=8)
    src_copy.wait()

    def gather_rows(row_index, first, count):
        for u in range(count):
            tmp[pl.ds(u * parts, parts), :] = big[pl.ds(src_sm[row_index, u], parts), :]
        for u in range(0, count, 16):
            for c in range(parts):
                send[pl.ds(pl.multiple_of(first + u, 16), 16), c * LANES:(c + 1) * LANES] = (
                    tmp[pl.ds(u * parts + c, 16, stride=parts), :].astype(BF16))

    def out_copy(index):
        rows_of = pl.ds(pl.multiple_of(index * cap, cap), cap)
        return pltpu.make_async_copy(send.at[rows_of], send_hbm.at[rows_of], out_sem)

    def gather_block(index, _):
        def gather(g, _):
            gather_rows(index * per_expert + g, pl.multiple_of(index * cap + g * LANES, 16), LANES)
            return 0

        lax.fori_loop(0, cap // LANES, gather, 0)
        if cap % LANES:
            gather_rows(index * per_expert + cap // LANES, pl.multiple_of(index * cap + cap // LANES * LANES, 16), cap % LANES)
        out_copy(index).start()
        return 0

    lax.fori_loop(0, num_experts, gather_block, 0)
    lax.fori_loop(0, num_experts, lambda index, _: (out_copy(index).wait(), 0)[1], 0)


def dispatch(tok_rows, ids, order, dims):
    size_b, size_x, cap = dims
    num_experts = 2 * size_b * size_x
    slots, slot_rows = num_experts * cap, num_experts * pl.cdiv(cap, LANES)
    tok_dev, width = tok_rows.shape
    rows, parts = tok_dev // LANES, width // LANES
    vmem, hbm = pl.BlockSpec(memory_space=pltpu.VMEM), pl.BlockSpec(memory_space=pltpu.HBM)
    dma = pltpu.SemaphoreType.DMA
    return pl.pallas_call(
        functools.partial(dispatch_kernel, dims),
        name="dispatch",
        out_shape=(jax.ShapeDtypeStruct((slots, width), BF16), jax.ShapeDtypeStruct(ids.shape, jnp.int32)),
        in_specs=[vmem, vmem, hbm],
        out_specs=(hbm, vmem),
        scratch_shapes=[
            pltpu.VMEM((rows, LANES), jnp.int32),
            pltpu.VMEM((rows, num_experts, 2 * LANES), F32),
            pltpu.VMEM((rows, LANES), jnp.int32),
            pltpu.VMEM((2 * slot_rows, rows * LANES), BF16),
            pltpu.VMEM((LANES, rows * LANES), BF16),
            pltpu.VMEM((slot_rows, LANES), jnp.int32),
            pltpu.SMEM((slot_rows, LANES), jnp.int32),
            pltpu.VMEM((tok_dev, width), BF16),
            pltpu.VMEM((tok_dev * parts + 8, LANES), F32),
            pltpu.VMEM((LANES * parts + 8, LANES), F32),
            pltpu.VMEM((slots, width), BF16),
            dma, dma, dma,
        ],
        compiler_params=pltpu.CompilerParams(vmem_limit_bytes=63 << 20),
        cost_estimate=pl.CostEstimate(flops=20_000_000_000, bytes_accessed=15_000_000, transcendentals=0),
    )(ids, order, tok_rows)


def pick(table, t):
    value = jnp.int32(0)
    for i, entry in enumerate(table):
        if entry:
            value = value + jnp.where(t == i, entry, 0)
    return value


def experts_kernel(dims, ids_ref, wr_ref, keys_ref, tau_ref, tok_hbm, send, w1_hbm, w2_hbm, w1_next, w2_next, w1_last, w2_last,
                   b1_hbm, b2_hbm, back_hbm, gate_ref, stage, recv, w1, w2, b1, b2,
                   tok_sem, wout_sem, win_sem, out_sem, in_sem, ret_sem, back_sem):
    size_b, size_x, cap = dims
    n = size_x
    rows = ids_ref.shape[0]
    num_experts = 2 * size_b * size_x
    tok_dev, chunk = tok_hbm.shape[0], stage.shape[1]
    i_dp, i_b, i_a = lax.axis_index("dp"), lax.axis_index("ep_b"), lax.axis_index("ep_a")
    pos_x, core, pos_y = i_a // 2, lax.rem(i_a, 2), i_b
    pos = (1 - core) * pos_x + core * pos_y
    wpos = (1 - core) * pos_y + core * pos_x

    def sends_to(kind, k):
        return i_dp, (1 - kind) * pos_y + kind * k, 2 * ((1 - kind) * k + kind * pos_x) + kind

    def serves(k, c):
        return i_dp, core * k + (1 - core) * pos_y, 2 * (core * pos_x + (1 - core) * k) + c

    def shares(k):
        return i_dp, (1 - core) * k + core * pos_y, 2 * ((1 - core) * pos_x + core * k) + core

    def block(i):
        return pl.ds(pl.multiple_of(i * cap, cap), cap)

    def fetch(q):
        return pltpu.make_async_copy(tok_hbm.at[pl.ds(pl.multiple_of(q * chunk, chunk), chunk)], stage.at[lax.rem(q, 2)],
                                     tok_sem.at[lax.rem(q, 2)])

    def each_chunk(body):
        chunks = tok_dev // chunk

        def step(q, _):
            @pl.when(q + 1 < chunks)
            def _():
                fetch(q + 1).start()
            fetch(q).wait()
            body(q, lax.rem(q, 2))
            return 0

        lax.fori_loop(0, chunks, step, 0)

    fetch(0).start()
    held = ((w1_hbm, w1), (w2_hbm, w2), (b1_hbm, b1), (b2_hbm, b2))
    arrived = {1: (w1_next, w2_next), n - 1: (w1_last, w2_last)}
    for i, (own, every) in enumerate(held):
        pltpu.make_async_copy(own, every.at[pl.ds(0, 1)], win_sem.at[i, 0]).start()
    for d, pair in arrived.items():
        for i, matrix in enumerate(pair):
            pltpu.make_async_copy(matrix, held[i][1].at[pl.ds(d, 1)], win_sem.at[i, d]).start()

    barrier = pltpu.get_barrier_semaphore()
    for k in range(n):
        for c in range(2):
            for device in (sends_to(c, k), serves(k, c)):
                pl.semaphore_signal(barrier, inc=1, device_id=device, device_id_type=MESH_ID)
    for d in range(1, n):
        pl.semaphore_signal(barrier, inc=1, device_id=shares(lax.rem(wpos + d, n)), device_id_type=MESH_ID)
    pl.semaphore_wait(barrier, 5 * n - 1)

    def weight_copy(i, d):
        own, every = held[i]
        return pltpu.make_async_remote_copy(
            src_ref=own, dst_ref=every.at[pl.ds(d, 1)], send_sem=wout_sem.at[i, d], recv_sem=win_sem.at[i, d],
            device_id=shares(lax.rem(wpos - d + n, n)), device_id_type=MESH_ID)

    near, far = [1, n - 1], list(range(2, n - 1))
    for d in near + far:
        for i in (2, 3):
            weight_copy(i, d).start()

    def passed_on(i):
        every = held[i][1]
        to = (wpos - 1 + n, wpos + 1)[i]
        return pltpu.make_async_remote_copy(
            src_ref=arrived[near[i]][i], dst_ref=every.at[pl.ds(2, 1)], send_sem=wout_sem.at[i, 2], recv_sem=win_sem.at[i, 2],
            device_id=shares(lax.rem(to, n)), device_id_type=MESH_ID)

    def weights_here(i, off):
        own, every = held[i]
        pltpu.make_async_copy(own, every.at[pl.ds(off, 1)], win_sem.at[i, off]).wait()

    iota_exp = iota((num_experts, LANES), 0)

    soon = [0] + near
    send_order = [(step, off, kind) for offs, group in ((soon, near), (soon, far), (soon, [0]), (far, near + far + [0]))
                  for off in offs for step in group for kind in range(2)]

    def outgoing(t):
        step, off, kind = (pick([e[i] for e in send_order], t) for i in range(3))
        k = lax.rem((1 - kind) * pos_x + kind * pos_y + step, n)
        j = lax.rem((1 - kind) * pos_y + kind * pos_x + off, n)
        return step, kind, k, j

    def send_block(t):
        step, kind, k, j = outgoing(t)
        src = (kind * n + k) * n + j
        dst = (((1 - kind) * pos_x + kind * pos_y) * n + j) * 2 + core
        own = (step == 0) & (kind == core)

        @pl.when(own)
        def _():
            pltpu.make_async_copy(send.at[block(src)], recv.at[block(dst)], in_sem.at[dst]).start()

        @pl.when(jnp.logical_not(own))
        def _():
            pltpu.make_async_remote_copy(
                src_ref=send.at[block(src)], dst_ref=recv.at[block(dst)], send_sem=out_sem.at[src], recv_sem=in_sem.at[dst],
                device_id=sends_to(kind, k), device_id_type=MESH_ID).start()

    blocks = 2 * n * n
    early = 2 * len(soon) * len(near)
    lax.fori_loop(0, early, lambda t, _: (send_block(t), 0)[1], 0)
    for i in range(2):
        passed_on(i).start()
    lax.fori_loop(early, blocks, lambda t, _: (send_block(t), 0)[1], 0)

    keys = keys_ref[...].astype(F32)
    key_unit = keys / jnp.sqrt(jnp.sum(keys * keys, axis=1, keepdims=True))
    tau = tau_ref[0, 0]
    key_pad = jnp.concatenate([key_unit, jnp.zeros((LANES - num_experts, key_unit.shape[1]), F32)], axis=0)
    span = chunk // LANES

    def gate_rows(i, slot):
        r = jnp.dot(stage[slot], wr_ref[...], preferred_element_type=F32)
        unit = r / jnp.sqrt(jnp.sum(r * r, axis=1, keepdims=True))
        dots = lax.dot_general(unit, key_pad, (((1,), (1,)), ((), ())), preferred_element_type=F32,
                               precision=lax.Precision.HIGHEST)
        logits = dots.T[:num_experts] / tau
        p = jnp.exp(logits - jnp.max(logits, axis=0, keepdims=True))
        total = jnp.sum(p, axis=0, keepdims=True)
        for q in range(span):
            mine = iota_exp == ids_ref[pl.ds(i * span + q, 1), :]
            cols = slice(q * LANES, (q + 1) * LANES)
            gate_ref[pl.ds(i * span + q, 1), :] = jnp.sum(jnp.where(mine, p[:, cols], 0.0), axis=0, keepdims=True) / total[:, cols]

    each_chunk(gate_rows)

    serve_order = ([(0, off) for off in soon] + [(step, off) for off in soon for step in near]
                   + [(step, off) for step in far for off in soon] + [(step, off) for off in far for step in near + far + [0]])
    first_use = [[int(off not in [o for _, o in serve_order[:t]])
                  for t, (_, off) in enumerate(serve_order)] for i in range(len(held))]

    def incoming(t):
        step, off = (pick([e[i] for e in serve_order], t) for i in range(2))
        return lax.rem(pos - step + n, n), off, lax.rem(wpos + off, n)

    def result_ends(t, c):
        k, _, j = incoming(t)
        src, dst = (k * n + j) * 2 + c, (core * n + pos) * n + j
        return k, src, dst, (k == pos) & (core == c)

    def send_results(t):
        for c in range(2):
            k, src, dst, own = result_ends(t, c)

            @pl.when(own)
            def _():
                pltpu.make_async_copy(recv.at[block(src)], back_hbm.at[block(dst)], back_sem.at[dst]).start()

            @pl.when(jnp.logical_not(own))
            def _():
                pltpu.make_async_remote_copy(
                    src_ref=recv.at[block(src)], dst_ref=back_hbm.at[block(dst)], send_sem=ret_sem.at[src],
                    recv_sem=back_sem.at[dst], device_id=serves(k, c), device_id_type=MESH_ID).start()

    def serve(t, _):
        k, off, j = incoming(t)
        first = (k * n + j) * 2

        for i in range(len(held)):
            @pl.when(pick(first_use[i], t) == 1)
            def _():
                weights_here(i, off)

        for c in range(2):
            pltpu.make_async_copy(send.at[block(0)], recv.at[block(first + c)], in_sem.at[first + c]).wait()
        here = pl.ds(pl.multiple_of(first * cap, 2 * cap), 2 * cap)
        hidden = jnp.dot(recv[here, :], w1[off], preferred_element_type=F32) + b1[off].astype(F32)
        hidden = (0.5 * hidden * (1.0 + lax.erf(hidden * (0.5 ** 0.5)))).astype(BF16)
        y = jnp.dot(hidden, w2[off], preferred_element_type=F32) + b2[off].astype(F32)
        recv[here, :] = y.astype(BF16)

        @pl.when(t > 0)
        def _():
            send_results(t - 1)
        return 0

    lax.fori_loop(0, n * n, serve, 0)
    send_results(jnp.int32(n * n - 1))

    for i in range(2):
        passed_on(i).wait_send()
        for d in near + far:
            weight_copy(2 + i, d).wait_send()

    def drain(t, _):
        sent = pltpu.make_async_remote_copy(
            src_ref=send.at[block(t)], dst_ref=recv.at[block(t)], send_sem=out_sem.at[t], recv_sem=in_sem.at[t],
            device_id=(i_dp, i_b, i_a), device_id_type=MESH_ID)
        returned = pltpu.make_async_remote_copy(
            src_ref=recv.at[block(t)], dst_ref=back_hbm.at[block(t)], send_sem=ret_sem.at[t], recv_sem=back_sem.at[t],
            device_id=(i_dp, i_b, i_a), device_id_type=MESH_ID)
        kind, k = t // (n * n), lax.rem(t // n, n)

        @pl.when((kind != core) | (k != pos))
        def _():
            sent.wait_send()

        @pl.when((t // (2 * n) != pos) | (lax.rem(t, 2) != core))
        def _():
            returned.wait_send()

        returned.wait_recv()
        return 0

    lax.fori_loop(0, blocks, drain, 0)


def experts(tok_rows, ids, send_rows, w_route, expert_keys, temperature, weights, b1, b2, dims):
    size_b, size_x, cap = dims
    n = size_x
    tok_dev, width = tok_rows.shape
    hidden = weights[0].shape[2]
    slots = send_rows.shape[0]
    vmem, smem, hbm = (pl.BlockSpec(memory_space=m) for m in (pltpu.VMEM, pltpu.SMEM, pltpu.HBM))
    dma = pltpu.SemaphoreType.DMA
    return pl.pallas_call(
        functools.partial(experts_kernel, dims),
        name="experts",
        out_shape=(jax.ShapeDtypeStruct((slots, width), BF16), jax.ShapeDtypeStruct(ids.shape, F32)),
        in_specs=[vmem] * 3 + [smem] + [hbm] * (4 + len(weights)),
        out_specs=(hbm, vmem),
        scratch_shapes=[
            pltpu.VMEM((2, min(tok_dev, 512), width), BF16),
            pltpu.VMEM((slots, width), BF16),
            pltpu.VMEM((n, width, hidden), BF16),
            pltpu.VMEM((n, hidden, width), BF16),
            pltpu.VMEM((n, 1, hidden), BF16),
            pltpu.VMEM((n, 1, width), BF16),
            dma((2,)), dma((4, n)), dma((4, n)),
            dma((2 * n * n,)), dma((2 * n * n,)), dma((2 * n * n,)), dma((2 * n * n,)),
        ],
        compiler_params=pltpu.CompilerParams(collective_id=1, has_side_effects=True, vmem_limit_bytes=61 << 20),
        cost_estimate=pl.CostEstimate(flops=4 * slots * width * hidden, bytes_accessed=30_000_000, transcendentals=0),
    )(ids, w_route, expert_keys, temperature.reshape(1, 1), tok_rows, send_rows, *weights, b1, b2)


def combine_kernel(back_hbm, dest_hbm, gate_hbm, out_ref, stage, big, tmp, dest_sm, gate_ref, sem, table_sem):
    i = pl.program_id(0)
    slots, width = back_hbm.shape
    parts = width // LANES
    chunk = stage.shape[1]
    chunks = slots // chunk

    @pl.when(i == 0)
    def _():
        def fetch(q):
            return pltpu.make_async_copy(back_hbm.at[pl.ds(pl.multiple_of(q * chunk, chunk), chunk)], stage.at[lax.rem(q, 2)],
                                         sem.at[lax.rem(q, 2)])
        fetch(0).start()
        tables = [pltpu.make_async_copy(dest_hbm, dest_sm, table_sem.at[0]), pltpu.make_async_copy(gate_hbm, gate_ref, table_sem.at[1])]
        for table in tables:
            table.start()
        big[pl.ds(slots * parts, 8), :] = jnp.zeros((8, LANES), F32)

        def widen_chunk(q, _):
            @pl.when(q + 1 < chunks)
            def _():
                fetch(q + 1).start()
            fetch(q).wait()

            def widen(u, _):
                base = pl.multiple_of(u * 16, 16)
                for c in range(parts):
                    big[pl.ds((q * chunk + base) * parts + c, 16, stride=parts), :] = (
                        stage[lax.rem(q, 2), pl.ds(base, 16), c * LANES:(c + 1) * LANES].astype(F32))
                return 0

            lax.fori_loop(0, chunk // 16, widen, 0, unroll=8)
            return 0

        lax.fori_loop(0, chunks, widen_chunk, 0)
        for table in tables:
            table.wait()

    def gather(g, _):
        row = i * (out_ref.shape[0] // LANES) + g
        for j in range(LANES):
            tmp[pl.ds(j * parts, parts), :] = big[pl.ds(dest_sm[row, j], parts), :]
        gate = jnp.broadcast_to(gate_ref[pl.ds(row, 1), :], (LANES, LANES)).T
        for j in range(0, LANES, 16):
            for c in range(parts):
                out_ref[pl.ds(pl.multiple_of(g * LANES + j, 16), 16), c * LANES:(c + 1) * LANES] = (
                    (gate[j:j + 16] * tmp[pl.ds(j * parts + c, 16, stride=parts), :]).astype(BF16))
        return 0

    lax.fori_loop(0, out_ref.shape[0] // LANES, gather, 0)


def combine(back_rows, dest, gate, tok_dev):
    slots, width = back_rows.shape
    parts = width // LANES
    block = 1024
    hbm = pl.BlockSpec(memory_space=pltpu.HBM)
    return pl.pallas_call(
        combine_kernel,
        name="combine",
        grid=(tok_dev // block,),
        out_shape=jax.ShapeDtypeStruct((tok_dev, width), BF16),
        in_specs=[hbm] * 3,
        out_specs=pl.BlockSpec((block, width), lambda i: (i, 0)),
        scratch_shapes=[
            pltpu.VMEM((2, 1280, width), BF16),
            pltpu.VMEM((slots * parts + 8, LANES), F32),
            pltpu.VMEM((LANES * parts + 8, LANES), F32),
            pltpu.SMEM(dest.shape, jnp.int32),
            pltpu.VMEM(gate.shape, F32),
            pltpu.SemaphoreType.DMA((2,)),
            pltpu.SemaphoreType.DMA((2,)),
        ],
        compiler_params=pltpu.CompilerParams(vmem_limit_bytes=61 << 20, dimension_semantics=("arbitrary",)),
        cost_estimate=pl.CostEstimate(flops=20_000_000_000, bytes_accessed=15_000_000, transcendentals=0),
    )(back_rows, dest, gate)


def solution(mesh):
    size_b, size_x = mesh.shape["ep_b"], mesh.shape["ep_a"] // 2
    num_experts = 2 * size_b * size_x
    tok_spec = P(("dp",) + EXPERT_AXES)
    expert_spec = P(EXPERT_AXES)

    def from_place(d, w):
        pairs = []
        for y in range(size_b):
            for x in range(size_x):
                pairs.append(((y * size_x + x) * 2, (((y - d) % size_b) * size_x + x) * 2))
                pairs.append(((y * size_x + x) * 2 + 1, (y * size_x + (x - d) % size_x) * 2 + 1))
        return lax.ppermute(w, EXPERT_AXES, pairs)

    def device_step(tokens, expert_ids, route_order, w_route, expert_keys, temperature, w_in, b_in, w_out, b_out):
        tok_dev = tokens.shape[1]
        cap = (5 * tok_dev + 4 * num_experts - 1) // (4 * num_experts)
        dims = (size_b, size_x, cap)
        ids = expert_ids.reshape(tok_dev // LANES, LANES)
        weights = [w_in, w_out] + [from_place(d, w) for d in (1, size_x - 1) for w in (w_in, w_out)]
        send_rows, dest = dispatch(tokens[0], ids, route_order.reshape(ids.shape), dims)
        back_rows, gate = experts(tokens[0], ids, send_rows, w_route, expert_keys, temperature, weights,
                                  b_in[:, None, :], b_out[:, None, :], dims)
        return combine(back_rows, dest, gate, tok_dev)[None]

    return jax.shard_map(
        device_step,
        mesh=mesh,
        in_specs=(tok_spec, tok_spec, tok_spec, P(), P(), P(), expert_spec, expert_spec, expert_spec, expert_spec),
        out_specs=tok_spec,
        check_vma=False,
    )
```

```python
import functools

import jax
import jax.numpy as jnp
from jax import lax
from jax.experimental import pallas as pl
from jax.experimental.pallas import tpu as pltpu
from jax.sharding import PartitionSpec as P

EXPERT_AXES = ("ep_b", "ep_a")
LANES = 128
MESH_ID = pl.DeviceIdType.MESH
F32 = jnp.float32
BF16 = jnp.bfloat16


def iota(shape, dim):
    return lax.broadcasted_iota(jnp.int32, shape, dim)


def dot_nt(a, b):
    return lax.dot_general(a, b, (((1,), (1,)), ((), ())), preferred_element_type=F32)


def as_bf16(mask):
    return jnp.where(mask, 1.0, 0.0).astype(BF16)


def virtual_expert(ids, size_b, size_x):
    i_b, i_a = ids // (2 * size_x), ids % (2 * size_x)
    x, core = i_a // 2, i_a % 2
    return jnp.where(core == 0, x * size_b + i_b, size_b * size_x + i_b * size_x + x)


def dispatch_kernel(dims, ids_ref, order_ref, tok_hbm, send_hbm, dest_ref,
                    rid_s, both_s, kept_s, hi_s, lo_s, src_vm, src_sm, tok_vm, big, tmp, send, tok_sem, src_sem, out_sem):
    size_b, size_x, cap = dims
    rows, slot_rows = ids_ref.shape[0], src_vm.shape[0]
    parts = tok_hbm.shape[1] // LANES
    tok_copy = pltpu.make_async_copy(tok_hbm, tok_vm, tok_sem)
    tok_copy.start()
    num_experts = 2 * size_b * size_x
    per_expert = slot_rows // num_experts
    upper = as_bf16((iota((LANES, 2 * LANES), 0) <= iota((LANES, 2 * LANES), 1)) | (iota((LANES, 2 * LANES), 1) >= LANES))
    ids_t = ids_ref[...].astype(F32).T.astype(BF16)
    iota_rows = iota((rows, LANES), 0)
    iota_lane = iota((LANES, LANES), 0)
    iota_exp = iota((num_experts, LANES), 0)
    iota_slot = iota((slot_rows, LANES), 0)
    zero_count = jnp.zeros((num_experts, LANES), F32)

    def row(r):
        return pl.ds(r, 1)

    def cols(r):
        return pl.ds(pl.multiple_of(r * LANES, LANES), LANES)

    def each(body, unroll):
        lax.fori_loop(0, rows, lambda r, _: (body(r), 0)[1], 0, unroll=unroll)

    def ranked_id(r):
        o = order_ref[row(r), :]
        table = jnp.dot(ids_t, as_bf16(iota_rows == o // LANES), preferred_element_type=F32)
        rid_s[row(r), :] = jnp.sum(jnp.where(iota_lane == o % LANES, table, 0.0), axis=0, keepdims=True).astype(jnp.int32)

    def ranked_count(r):
        both_s[r] = jnp.dot(as_bf16(iota_exp == rid_s[row(r), :]), upper, preferred_element_type=F32)

    def position(mine, r, count):
        return jnp.sum(jnp.where(mine, both_s[r, :, :LANES] + count, 0.0), axis=0, keepdims=True)

    def ranked_kept(r, count):
        rank = position(iota_exp == rid_s[row(r), :], r, count)
        kept_s[row(r), :] = (rank <= float(cap)).astype(jnp.int32)
        return count + both_s[r, :, LANES:]

    def scatter_kept(r):
        o = order_ref[row(r), :]
        hi_s[:rows, cols(r)] = as_bf16((iota_rows == o // LANES) & (kept_s[row(r), :] > 0))
        lo_s[:, cols(r)] = as_bf16(iota_lane == o % LANES)

    each(ranked_id, 16)
    each(ranked_count, 16)
    lax.fori_loop(0, rows, ranked_kept, zero_count, unroll=8)
    each(scatter_kept, 8)
    kept_s[...] = dot_nt(hi_s[:rows, :], lo_s[...]).astype(jnp.int32)

    def expert_of(r):
        return virtual_expert(ids_ref[row(r), :], size_b, size_x)

    def mine_kept(r):
        return (iota_exp == expert_of(r)) & (kept_s[row(r), :] > 0)

    def token_count(r):
        both_s[r] = jnp.dot(as_bf16(mine_kept(r)), upper, preferred_element_type=F32)

    lane = iota((1, LANES), 1).astype(F32)

    def placed(r, count):
        place = position(mine_kept(r), r, count).astype(jnp.int32) - 1
        kept = kept_s[row(r), :] > 0
        expert = expert_of(r)
        dest_ref[row(r), :] = jnp.where(kept, expert * cap + place, num_experts * cap) * parts
        rid_s[row(r), :] = jnp.where(kept, expert * (per_expert * LANES) + place, slot_rows * LANES)
        return count + both_s[r, :, LANES:]

    def scatter_source(r):
        slot = rid_s[row(r), :]
        hit = jnp.where(iota_slot == slot // LANES, 1.0, 0.0)
        hi_s[:slot_rows, cols(r)] = (hit * lax.convert_element_type(r, F32)).astype(BF16)
        hi_s[slot_rows:, cols(r)] = (hit * lane).astype(BF16)
        lo_s[:, cols(r)] = as_bf16(iota_lane == slot % LANES)

    each(token_count, 16)
    lax.fori_loop(0, rows, placed, zero_count, unroll=8)
    each(scatter_source, 8)
    found = dot_nt(hi_s[...], lo_s[...])
    src_vm[...] = ((found[:slot_rows] * float(LANES) + found[slot_rows:]) * float(parts)).astype(jnp.int32)
    src_copy = pltpu.make_async_copy(src_vm, src_sm, src_sem)
    src_copy.start()

    tok_copy.wait()

    def widen(i, _):
        base = pl.multiple_of(i * 16, 16)
        for c in range(parts):
            big[pl.ds(base * parts + c, 16, stride=parts), :] = tok_vm[pl.ds(base, 16), c * LANES:(c + 1) * LANES].astype(F32)
        return 0

    lax.fori_loop(0, tok_vm.shape[0] // 16, widen, 0, unroll=8)
    src_copy.wait()

    def gather_rows(row_index, first, count):
        for u in range(count):
            tmp[pl.ds(u * parts, parts), :] = big[pl.ds(src_sm[row_index, u], parts), :]
        for u in range(0, count, 16):
            for c in range(parts):
                send[pl.ds(pl.multiple_of(first + u, 16), 16), c * LANES:(c + 1) * LANES] = (
                    tmp[pl.ds(u * parts + c, 16, stride=parts), :].astype(BF16))

    def out_copy(index):
        rows_of = pl.ds(pl.multiple_of(index * cap, cap), cap)
        return pltpu.make_async_copy(send.at[rows_of], send_hbm.at[rows_of], out_sem)

    def gather_block(index, _):
        def gather(g, _):
            gather_rows(index * per_expert + g, pl.multiple_of(index * cap + g * LANES, 16), LANES)
            return 0

        lax.fori_loop(0, cap // LANES, gather, 0)
        if cap % LANES:
            gather_rows(index * per_expert + cap // LANES, pl.multiple_of(index * cap + cap // LANES * LANES, 16), cap % LANES)
        out_copy(index).start()
        return 0

    lax.fori_loop(0, num_experts, gather_block, 0)
    lax.fori_loop(0, num_experts, lambda index, _: (out_copy(index).wait(), 0)[1], 0)


def dispatch(tok_rows, ids, order, dims):
    size_b, size_x, cap = dims
    num_experts = 2 * size_b * size_x
    slots, slot_rows = num_experts * cap, num_experts * pl.cdiv(cap, LANES)
    tok_dev, width = tok_rows.shape
    rows, parts = tok_dev // LANES, width // LANES
    vmem, hbm = pl.BlockSpec(memory_space=pltpu.VMEM), pl.BlockSpec(memory_space=pltpu.HBM)
    dma = pltpu.SemaphoreType.DMA
    return pl.pallas_call(
        functools.partial(dispatch_kernel, dims),
        name="dispatch",
        out_shape=(jax.ShapeDtypeStruct((slots, width), BF16), jax.ShapeDtypeStruct(ids.shape, jnp.int32)),
        in_specs=[vmem, vmem, hbm],
        out_specs=(hbm, vmem),
        scratch_shapes=[
            pltpu.VMEM((rows, LANES), jnp.int32),
            pltpu.VMEM((rows, num_experts, 2 * LANES), F32),
            pltpu.VMEM((rows, LANES), jnp.int32),
            pltpu.VMEM((2 * slot_rows, rows * LANES), BF16),
            pltpu.VMEM((LANES, rows * LANES), BF16),
            pltpu.VMEM((slot_rows, LANES), jnp.int32),
            pltpu.SMEM((slot_rows, LANES), jnp.int32),
            pltpu.VMEM((tok_dev, width), BF16),
            pltpu.VMEM((tok_dev * parts + 8, LANES), F32),
            pltpu.VMEM((LANES * parts + 8, LANES), F32),
            pltpu.VMEM((slots, width), BF16),
            dma, dma, dma,
        ],
        compiler_params=pltpu.CompilerParams(vmem_limit_bytes=63 << 20),
        cost_estimate=pl.CostEstimate(flops=20_000_000_000, bytes_accessed=15_000_000, transcendentals=0),
    )(ids, order, tok_rows)


def pick(table, t):
    value = jnp.int32(0)
    for i, entry in enumerate(table):
        if entry:
            value = value + jnp.where(t == i, entry, 0)
    return value


def experts_kernel(dims, ids_ref, wr_ref, keys_ref, tau_ref, tok_hbm, send, w1_hbm, w2_hbm, w1_next, w2_next, w1_last, w2_last,
                   b1_hbm, b2_hbm, back_hbm, gate_ref, stage, recv, w1, w2, b1, b2,
                   tok_sem, wout_sem, win_sem, out_sem, in_sem, ret_sem, back_sem):
    size_b, size_x, cap = dims
    n = size_x
    rows = ids_ref.shape[0]
    num_experts = 2 * size_b * size_x
    tok_dev, chunk = tok_hbm.shape[0], stage.shape[1]
    i_dp, i_b, i_a = lax.axis_index("dp"), lax.axis_index("ep_b"), lax.axis_index("ep_a")
    pos_x, core, pos_y = i_a // 2, lax.rem(i_a, 2), i_b
    pos = (1 - core) * pos_x + core * pos_y
    wpos = (1 - core) * pos_y + core * pos_x

    def sends_to(kind, k):
        return i_dp, (1 - kind) * pos_y + kind * k, 2 * ((1 - kind) * k + kind * pos_x) + kind

    def serves(k, c):
        return i_dp, core * k + (1 - core) * pos_y, 2 * (core * pos_x + (1 - core) * k) + c

    def shares(k):
        return i_dp, (1 - core) * k + core * pos_y, 2 * ((1 - core) * pos_x + core * k) + core

    def block(i):
        return pl.ds(pl.multiple_of(i * cap, cap), cap)

    def fetch(q):
        return pltpu.make_async_copy(tok_hbm.at[pl.ds(pl.multiple_of(q * chunk, chunk), chunk)], stage.at[lax.rem(q, 2)],
                                     tok_sem.at[lax.rem(q, 2)])

    def each_chunk(body):
        chunks = tok_dev // chunk

        def step(q, _):
            @pl.when(q + 1 < chunks)
            def _():
                fetch(q + 1).start()
            fetch(q).wait()
            body(q, lax.rem(q, 2))
            return 0

        lax.fori_loop(0, chunks, step, 0)

    fetch(0).start()
    held = ((w1_hbm, w1), (w2_hbm, w2), (b1_hbm, b1), (b2_hbm, b2))
    arrived = {1: (w1_next, w2_next), n - 1: (w1_last, w2_last)}
    for i, (own, every) in enumerate(held):
        pltpu.make_async_copy(own, every.at[pl.ds(0, 1)], win_sem.at[i, 0]).start()
    for d, pair in arrived.items():
        for i, matrix in enumerate(pair):
            pltpu.make_async_copy(matrix, held[i][1].at[pl.ds(d, 1)], win_sem.at[i, d]).start()

    barrier = pltpu.get_barrier_semaphore()
    for k in range(n):
        for c in range(2):
            for device in (sends_to(c, k), serves(k, c)):
                pl.semaphore_signal(barrier, inc=1, device_id=device, device_id_type=MESH_ID)
    for d in range(1, n):
        pl.semaphore_signal(barrier, inc=1, device_id=shares(lax.rem(wpos + d, n)), device_id_type=MESH_ID)
    pl.semaphore_wait(barrier, 5 * n - 1)

    def weight_copy(i, d):
        own, every = held[i]
        return pltpu.make_async_remote_copy(
            src_ref=own, dst_ref=every.at[pl.ds(d, 1)], send_sem=wout_sem.at[i, d], recv_sem=win_sem.at[i, d],
            device_id=shares(lax.rem(wpos - d + n, n)), device_id_type=MESH_ID)

    near, far = [1, n - 1], list(range(2, n - 1))
    for d in near + far:
        for i in (2, 3):
            weight_copy(i, d).start()

    def passed_on(i):
        every = held[i][1]
        to = (wpos - 1 + n, wpos + 1)[i]
        return pltpu.make_async_remote_copy(
            src_ref=arrived[near[i]][i], dst_ref=every.at[pl.ds(2, 1)], send_sem=wout_sem.at[i, 2], recv_sem=win_sem.at[i, 2],
            device_id=shares(lax.rem(to, n)), device_id_type=MESH_ID)

    def weights_here(i, off):
        own, every = held[i]
        pltpu.make_async_copy(own, every.at[pl.ds(off, 1)], win_sem.at[i, off]).wait()

    iota_exp = iota((num_experts, LANES), 0)

    soon = [0] + near
    send_order = [(step, off, kind) for offs, group in ((soon, near), (soon, far), (soon, [0]), (far, near + far + [0]))
                  for off in offs for step in group for kind in range(2)]

    def outgoing(t):
        step, off, kind = (pick([e[i] for e in send_order], t) for i in range(3))
        k = lax.rem((1 - kind) * pos_x + kind * pos_y + step, n)
        j = lax.rem((1 - kind) * pos_y + kind * pos_x + off, n)
        return step, kind, k, j

    def send_block(t):
        step, kind, k, j = outgoing(t)
        src = (kind * n + k) * n + j
        dst = (((1 - kind) * pos_x + kind * pos_y) * n + j) * 2 + core
        own = (step == 0) & (kind == core)

        @pl.when(own)
        def _():
            pltpu.make_async_copy(send.at[block(src)], recv.at[block(dst)], in_sem.at[dst]).start()

        @pl.when(jnp.logical_not(own))
        def _():
            pltpu.make_async_remote_copy(
                src_ref=send.at[block(src)], dst_ref=recv.at[block(dst)], send_sem=out_sem.at[src], recv_sem=in_sem.at[dst],
                device_id=sends_to(kind, k), device_id_type=MESH_ID).start()

    blocks = 2 * n * n
    early = 2 * len(soon) * len(near)
    lax.fori_loop(0, early, lambda t, _: (send_block(t), 0)[1], 0)
    for i in range(2):
        passed_on(i).start()
    lax.fori_loop(early, blocks, lambda t, _: (send_block(t), 0)[1], 0)

    keys = keys_ref[...].astype(F32)
    key_unit = keys / jnp.sqrt(jnp.sum(keys * keys, axis=1, keepdims=True))
    tau = tau_ref[0, 0]
    key_pad = jnp.concatenate([key_unit, jnp.zeros((LANES - num_experts, key_unit.shape[1]), F32)], axis=0)
    span = chunk // LANES

    def gate_rows(i, slot):
        r = jnp.dot(stage[slot], wr_ref[...], preferred_element_type=F32)
        unit = r / jnp.sqrt(jnp.sum(r * r, axis=1, keepdims=True))
        dots = lax.dot_general(unit, key_pad, (((1,), (1,)), ((), ())), preferred_element_type=F32,
                               precision=lax.Precision.HIGHEST)
        logits = dots.T[:num_experts] / tau
        p = jnp.exp(logits - jnp.max(logits, axis=0, keepdims=True))
        total = jnp.sum(p, axis=0, keepdims=True)
        for q in range(span):
            mine = iota_exp == ids_ref[pl.ds(i * span + q, 1), :]
            cols = slice(q * LANES, (q + 1) * LANES)
            gate_ref[pl.ds(i * span + q, 1), :] = jnp.sum(jnp.where(mine, p[:, cols], 0.0), axis=0, keepdims=True) / total[:, cols]

    each_chunk(gate_rows)

    serve_order = ([(0, off) for off in soon] + [(step, off) for off in soon for step in near]
                   + [(step, off) for step in far for off in soon] + [(step, off) for off in far for step in near + far + [0]])
    first_use = [[int(off not in [o for _, o in serve_order[:t]])
                  for t, (_, off) in enumerate(serve_order)] for i in range(len(held))]

    def incoming(t):
        step, off = (pick([e[i] for e in serve_order], t) for i in range(2))
        return lax.rem(pos - step + n, n), off, lax.rem(wpos + off, n)

    def result_ends(t, c):
        k, _, j = incoming(t)
        src, dst = (k * n + j) * 2 + c, (core * n + pos) * n + j
        return k, src, dst, (k == pos) & (core == c)

    def send_results(t):
        for c in range(2):
            k, src, dst, own = result_ends(t, c)

            @pl.when(own)
            def _():
                pltpu.make_async_copy(recv.at[block(src)], back_hbm.at[block(dst)], back_sem.at[dst]).start()

            @pl.when(jnp.logical_not(own))
            def _():
                pltpu.make_async_remote_copy(
                    src_ref=recv.at[block(src)], dst_ref=back_hbm.at[block(dst)], send_sem=ret_sem.at[src],
                    recv_sem=back_sem.at[dst], device_id=serves(k, c), device_id_type=MESH_ID).start()

    def serve(t, _):
        k, off, j = incoming(t)
        first = (k * n + j) * 2

        for i in range(len(held)):
            @pl.when(pick(first_use[i], t) == 1)
            def _():
                weights_here(i, off)

        for c in range(2):
            pltpu.make_async_copy(send.at[block(0)], recv.at[block(first + c)], in_sem.at[first + c]).wait()
        here = pl.ds(pl.multiple_of(first * cap, 2 * cap), 2 * cap)
        hidden = jnp.dot(recv[here, :], w1[off], preferred_element_type=F32) + b1[off].astype(F32)
        hidden = (0.5 * hidden * (1.0 + lax.erf(hidden * (0.5 ** 0.5)))).astype(BF16)
        y = jnp.dot(hidden, w2[off], preferred_element_type=F32) + b2[off].astype(F32)
        recv[here, :] = y.astype(BF16)

        @pl.when(t > 0)
        def _():
            send_results(t - 1)
        return 0

    lax.fori_loop(0, n * n, serve, 0)
    send_results(jnp.int32(n * n - 1))

    for i in range(2):
        passed_on(i).wait_send()
        for d in near + far:
            weight_copy(2 + i, d).wait_send()

    def drain(t, _):
        sent = pltpu.make_async_remote_copy(
            src_ref=send.at[block(t)], dst_ref=recv.at[block(t)], send_sem=out_sem.at[t], recv_sem=in_sem.at[t],
            device_id=(i_dp, i_b, i_a), device_id_type=MESH_ID)
        returned = pltpu.make_async_remote_copy(
            src_ref=recv.at[block(t)], dst_ref=back_hbm.at[block(t)], send_sem=ret_sem.at[t], recv_sem=back_sem.at[t],
            device_id=(i_dp, i_b, i_a), device_id_type=MESH_ID)
        kind, k = t // (n * n), lax.rem(t // n, n)

        @pl.when((kind != core) | (k != pos))
        def _():
            sent.wait_send()

        @pl.when((t // (2 * n) != pos) | (lax.rem(t, 2) != core))
        def _():
            returned.wait_send()

        returned.wait_recv()
        return 0

    lax.fori_loop(0, blocks, drain, 0)


def experts(tok_rows, ids, send_rows, w_route, expert_keys, temperature, weights, b1, b2, dims):
    size_b, size_x, cap = dims
    n = size_x
    tok_dev, width = tok_rows.shape
    hidden = weights[0].shape[2]
    slots = send_rows.shape[0]
    vmem, smem, hbm = (pl.BlockSpec(memory_space=m) for m in (pltpu.VMEM, pltpu.SMEM, pltpu.HBM))
    dma = pltpu.SemaphoreType.DMA
    return pl.pallas_call(
        functools.partial(experts_kernel, dims),
        name="experts",
        out_shape=(jax.ShapeDtypeStruct((slots, width), BF16), jax.ShapeDtypeStruct(ids.shape, F32)),
        in_specs=[vmem] * 3 + [smem] + [hbm] * (4 + len(weights)),
        out_specs=(hbm, vmem),
        scratch_shapes=[
            pltpu.VMEM((2, min(tok_dev, 512), width), BF16),
            pltpu.VMEM((slots, width), BF16),
            pltpu.VMEM((n, width, hidden), BF16),
            pltpu.VMEM((n, hidden, width), BF16),
            pltpu.VMEM((n, 1, hidden), BF16),
            pltpu.VMEM((n, 1, width), BF16),
            dma((2,)), dma((4, n)), dma((4, n)),
            dma((2 * n * n,)), dma((2 * n * n,)), dma((2 * n * n,)), dma((2 * n * n,)),
        ],
        compiler_params=pltpu.CompilerParams(collective_id=1, has_side_effects=True, vmem_limit_bytes=61 << 20),
        cost_estimate=pl.CostEstimate(flops=4 * slots * width * hidden, bytes_accessed=30_000_000, transcendentals=0),
    )(ids, w_route, expert_keys, temperature.reshape(1, 1), tok_rows, send_rows, *weights, b1, b2)


def combine_kernel(back_hbm, dest_hbm, gate_hbm, out_ref, stage, big, tmp, dest_sm, gate_ref, sem, table_sem):
    i = pl.program_id(0)
    slots, width = back_hbm.shape
    parts = width // LANES
    chunk = stage.shape[1]
    chunks = slots // chunk

    @pl.when(i == 0)
    def _():
        def fetch(q):
            return pltpu.make_async_copy(back_hbm.at[pl.ds(pl.multiple_of(q * chunk, chunk), chunk)], stage.at[q], sem.at[q])

        for q in range(chunks):
            fetch(q).start()
        tables = [pltpu.make_async_copy(dest_hbm, dest_sm, table_sem.at[0]), pltpu.make_async_copy(gate_hbm, gate_ref, table_sem.at[1])]
        for table in tables:
            table.start()
        big[pl.ds(slots * parts, 8), :] = jnp.zeros((8, LANES), F32)

        def widen_chunk(q, _):
            fetch(q).wait()

            def widen(u, _):
                base = pl.multiple_of(u * 16, 16)
                for c in range(parts):
                    big[pl.ds((q * chunk + base) * parts + c, 16, stride=parts), :] = (
                        stage[q, pl.ds(base, 16), c * LANES:(c + 1) * LANES].astype(F32))
                return 0

            lax.fori_loop(0, chunk // 16, widen, 0, unroll=8)
            return 0

        lax.fori_loop(0, chunks, widen_chunk, 0)
        for table in tables:
            table.wait()

    def gather(g, _):
        row = i * (out_ref.shape[0] // LANES) + g
        for j in range(LANES):
            tmp[pl.ds(j * parts, parts), :] = big[pl.ds(dest_sm[row, j], parts), :]
        gate = jnp.broadcast_to(gate_ref[pl.ds(row, 1), :], (LANES, LANES)).T
        for j in range(0, LANES, 16):
            for c in range(parts):
                out_ref[pl.ds(pl.multiple_of(g * LANES + j, 16), 16), c * LANES:(c + 1) * LANES] = (
                    (gate[j:j + 16] * tmp[pl.ds(j * parts + c, 16, stride=parts), :]).astype(BF16))
        return 0

    lax.fori_loop(0, out_ref.shape[0] // LANES, gather, 0)


def combine(back_rows, dest, gate, tok_dev):
    slots, width = back_rows.shape
    parts = width // LANES
    block = 1024
    hbm = pl.BlockSpec(memory_space=pltpu.HBM)
    return pl.pallas_call(
        combine_kernel,
        name="combine",
        grid=(tok_dev // block,),
        out_shape=jax.ShapeDtypeStruct((tok_dev, width), BF16),
        in_specs=[hbm] * 3,
        out_specs=pl.BlockSpec((block, width), lambda i: (i, 0)),
        scratch_shapes=[
            pltpu.VMEM((8, slots // 8, width), BF16),
            pltpu.VMEM((slots * parts + 8, LANES), F32),
            pltpu.VMEM((LANES * parts + 8, LANES), F32),
            pltpu.SMEM(dest.shape, jnp.int32),
            pltpu.VMEM(gate.shape, F32),
            pltpu.SemaphoreType.DMA((8,)),
            pltpu.SemaphoreType.DMA((2,)),
        ],
        compiler_params=pltpu.CompilerParams(vmem_limit_bytes=61 << 20, dimension_semantics=("arbitrary",)),
        cost_estimate=pl.CostEstimate(flops=20_000_000_000, bytes_accessed=15_000_000, transcendentals=0),
    )(back_rows, dest, gate)


def solution(mesh):
    size_b, size_x = mesh.shape["ep_b"], mesh.shape["ep_a"] // 2
    num_experts = 2 * size_b * size_x
    tok_spec = P(("dp",) + EXPERT_AXES)
    expert_spec = P(EXPERT_AXES)

    def from_place(d, w):
        pairs = []
        for y in range(size_b):
            for x in range(size_x):
                pairs.append(((y * size_x + x) * 2, (((y - d) % size_b) * size_x + x) * 2))
                pairs.append(((y * size_x + x) * 2 + 1, (y * size_x + (x - d) % size_x) * 2 + 1))
        return lax.ppermute(w, EXPERT_AXES, pairs)

    def device_step(tokens, expert_ids, route_order, w_route, expert_keys, temperature, w_in, b_in, w_out, b_out):
        tok_dev = tokens.shape[1]
        cap = (5 * tok_dev + 4 * num_experts - 1) // (4 * num_experts)
        dims = (size_b, size_x, cap)
        ids = expert_ids.reshape(tok_dev // LANES, LANES)
        weights = [w_in, w_out] + [from_place(d, w) for d in (1, size_x - 1) for w in (w_in, w_out)]
        send_rows, dest = dispatch(tokens[0], ids, route_order.reshape(ids.shape), dims)
        back_rows, gate = experts(tokens[0], ids, send_rows, w_route, expert_keys, temperature, weights,
                                  b_in[:, None, :], b_out[:, None, :], dims)
        return combine(back_rows, dest, gate, tok_dev)[None]

    return jax.shard_map(
        device_step,
        mesh=mesh,
        in_specs=(tok_spec, tok_spec, tok_spec, P(), P(), P(), expert_spec, expert_spec, expert_spec, expert_spec),
        out_specs=tok_spec,
        check_vma=False,
    )
```

```python
import functools

import jax
import jax.numpy as jnp
from jax import lax
from jax.experimental import pallas as pl
from jax.experimental.pallas import tpu as pltpu
from jax.sharding import PartitionSpec as P

EXPERT_AXES = ("ep_b", "ep_a")
LANES = 128
MESH_ID = pl.DeviceIdType.MESH
F32 = jnp.float32
BF16 = jnp.bfloat16


def iota(shape, dim):
    return lax.broadcasted_iota(jnp.int32, shape, dim)


def dot_nt(a, b):
    return lax.dot_general(a, b, (((1,), (1,)), ((), ())), preferred_element_type=F32)


def as_bf16(mask):
    return jnp.where(mask, 1.0, 0.0).astype(BF16)


def virtual_expert(ids, size_b, size_x):
    i_b, i_a = ids // (2 * size_x), ids % (2 * size_x)
    x, core = i_a // 2, i_a % 2
    return jnp.where(core == 0, x * size_b + i_b, size_b * size_x + i_b * size_x + x)


def dispatch_kernel(dims, ids_ref, order_ref, tok_hbm, send_hbm, dest_ref,
                    rid_s, both_s, kept_s, hi_s, lo_s, src_vm, src_sm, tok_vm, big, tmp, send, tok_sem, src_sem, out_sem):
    size_b, size_x, cap = dims
    rows, slot_rows = ids_ref.shape[0], src_vm.shape[0]
    parts = tok_hbm.shape[1] // LANES
    tok_copy = pltpu.make_async_copy(tok_hbm, tok_vm, tok_sem)
    tok_copy.start()
    num_experts = 2 * size_b * size_x
    per_expert = slot_rows // num_experts
    upper = as_bf16((iota((LANES, 2 * LANES), 0) <= iota((LANES, 2 * LANES), 1)) | (iota((LANES, 2 * LANES), 1) >= LANES))
    ids_t = ids_ref[...].astype(F32).T.astype(BF16)
    iota_rows = iota((rows, LANES), 0)
    iota_lane = iota((LANES, LANES), 0)
    iota_exp = iota((num_experts, LANES), 0)
    iota_slot = iota((slot_rows, LANES), 0)
    zero_count = jnp.zeros((num_experts, LANES), F32)

    def row(r):
        return pl.ds(r, 1)

    def cols(r):
        return pl.ds(pl.multiple_of(r * LANES, LANES), LANES)

    def each(body, unroll):
        lax.fori_loop(0, rows, lambda r, _: (body(r), 0)[1], 0, unroll=unroll)

    def ranked_id(r):
        o = order_ref[row(r), :]
        table = jnp.dot(ids_t, as_bf16(iota_rows == o // LANES), preferred_element_type=F32)
        rid_s[row(r), :] = jnp.sum(jnp.where(iota_lane == o % LANES, table, 0.0), axis=0, keepdims=True).astype(jnp.int32)

    def ranked_count(r):
        both_s[r] = jnp.dot(as_bf16(iota_exp == rid_s[row(r), :]), upper, preferred_element_type=F32)

    def position(mine, r, count):
        return jnp.sum(jnp.where(mine, both_s[r, :, :LANES] + count, 0.0), axis=0, keepdims=True)

    def ranked_kept(r, count):
        rank = position(iota_exp == rid_s[row(r), :], r, count)
        kept_s[row(r), :] = (rank <= float(cap)).astype(jnp.int32)
        return count + both_s[r, :, LANES:]

    def scatter_kept(r):
        o = order_ref[row(r), :]
        hi_s[:rows, cols(r)] = as_bf16((iota_rows == o // LANES) & (kept_s[row(r), :] > 0))
        lo_s[:, cols(r)] = as_bf16(iota_lane == o % LANES)

    each(ranked_id, 16)
    each(ranked_count, 16)
    lax.fori_loop(0, rows, ranked_kept, zero_count, unroll=8)
    each(scatter_kept, 8)
    kept_s[...] = dot_nt(hi_s[:rows, :], lo_s[...]).astype(jnp.int32)

    def expert_of(r):
        return virtual_expert(ids_ref[row(r), :], size_b, size_x)

    def mine_kept(r):
        return (iota_exp == expert_of(r)) & (kept_s[row(r), :] > 0)

    def token_count(r):
        both_s[r] = jnp.dot(as_bf16(mine_kept(r)), upper, preferred_element_type=F32)

    lane = iota((1, LANES), 1).astype(F32)

    def placed(r, count):
        place = position(mine_kept(r), r, count).astype(jnp.int32) - 1
        kept = kept_s[row(r), :] > 0
        expert = expert_of(r)
        dest_ref[row(r), :] = jnp.where(kept, expert * cap + place, num_experts * cap) * parts
        rid_s[row(r), :] = jnp.where(kept, expert * (per_expert * LANES) + place, slot_rows * LANES)
        return count + both_s[r, :, LANES:]

    def scatter_source(r):
        slot = rid_s[row(r), :]
        hit = jnp.where(iota_slot == slot // LANES, 1.0, 0.0)
        hi_s[:slot_rows, cols(r)] = (hit * lax.convert_element_type(r, F32)).astype(BF16)
        hi_s[slot_rows:, cols(r)] = (hit * lane).astype(BF16)
        lo_s[:, cols(r)] = as_bf16(iota_lane == slot % LANES)

    each(token_count, 16)
    lax.fori_loop(0, rows, placed, zero_count, unroll=8)
    each(scatter_source, 8)
    found = dot_nt(hi_s[...], lo_s[...])
    src_vm[...] = ((found[:slot_rows] * float(LANES) + found[slot_rows:]) * float(parts)).astype(jnp.int32)
    src_copy = pltpu.make_async_copy(src_vm, src_sm, src_sem)
    src_copy.start()

    tok_copy.wait()

    def widen(i, _):
        base = pl.multiple_of(i * 16, 16)
        for c in range(parts):
            big[pl.ds(base * parts + c, 16, stride=parts), :] = tok_vm[pl.ds(base, 16), c * LANES:(c + 1) * LANES].astype(F32)
        return 0

    lax.fori_loop(0, tok_vm.shape[0] // 16, widen, 0, unroll=8)
    src_copy.wait()

    def gather_rows(row_index, first, count):
        for u in range(count):
            tmp[pl.ds(u * parts, parts), :] = big[pl.ds(src_sm[row_index, u], parts), :]
        for u in range(0, count, 16):
            for c in range(parts):
                send[pl.ds(pl.multiple_of(first + u, 16), 16), c * LANES:(c + 1) * LANES] = (
                    tmp[pl.ds(u * parts + c, 16, stride=parts), :].astype(BF16))

    def out_copy(index):
        rows_of = pl.ds(pl.multiple_of(index * cap, cap), cap)
        return pltpu.make_async_copy(send.at[rows_of], send_hbm.at[rows_of], out_sem)

    def gather_block(index, _):
        def gather(g, _):
            gather_rows(index * per_expert + g, pl.multiple_of(index * cap + g * LANES, 16), LANES)
            return 0

        lax.fori_loop(0, cap // LANES, gather, 0)
        if cap % LANES:
            gather_rows(index * per_expert + cap // LANES, pl.multiple_of(index * cap + cap // LANES * LANES, 16), cap % LANES)
        out_copy(index).start()
        return 0

    lax.fori_loop(0, num_experts, gather_block, 0)
    lax.fori_loop(0, num_experts, lambda index, _: (out_copy(index).wait(), 0)[1], 0)


def dispatch(tok_rows, ids, order, dims):
    size_b, size_x, cap = dims
    num_experts = 2 * size_b * size_x
    slots, slot_rows = num_experts * cap, num_experts * pl.cdiv(cap, LANES)
    tok_dev, width = tok_rows.shape
    rows, parts = tok_dev // LANES, width // LANES
    vmem, hbm = pl.BlockSpec(memory_space=pltpu.VMEM), pl.BlockSpec(memory_space=pltpu.HBM)
    dma = pltpu.SemaphoreType.DMA
    return pl.pallas_call(
        functools.partial(dispatch_kernel, dims),
        name="dispatch",
        out_shape=(jax.ShapeDtypeStruct((slots, width), BF16), jax.ShapeDtypeStruct(ids.shape, jnp.int32)),
        in_specs=[vmem, vmem, hbm],
        out_specs=(hbm, vmem),
        scratch_shapes=[
            pltpu.VMEM((rows, LANES), jnp.int32),
            pltpu.VMEM((rows, num_experts, 2 * LANES), F32),
            pltpu.VMEM((rows, LANES), jnp.int32),
            pltpu.VMEM((2 * slot_rows, rows * LANES), BF16),
            pltpu.VMEM((LANES, rows * LANES), BF16),
            pltpu.VMEM((slot_rows, LANES), jnp.int32),
            pltpu.SMEM((slot_rows, LANES), jnp.int32),
            pltpu.VMEM((tok_dev, width), BF16),
            pltpu.VMEM((tok_dev * parts + 8, LANES), F32),
            pltpu.VMEM((LANES * parts + 8, LANES), F32),
            pltpu.VMEM((slots, width), BF16),
            dma, dma, dma,
        ],
        compiler_params=pltpu.CompilerParams(vmem_limit_bytes=63 << 20),
        cost_estimate=pl.CostEstimate(flops=20_000_000_000, bytes_accessed=15_000_000, transcendentals=0),
    )(ids, order, tok_rows)


def pick(table, t):
    value = jnp.int32(0)
    for i, entry in enumerate(table):
        if entry:
            value = value + jnp.where(t == i, entry, 0)
    return value


def experts_kernel(dims, ids_ref, wr_ref, keys_ref, tau_ref, tok_hbm, send, w1_hbm, w2_hbm, w1_next, w2_next, w1_last, w2_last,
                   b1_hbm, b2_hbm, back_hbm, gate_ref, stage, recv, w1, w2, b1, b2,
                   tok_sem, wout_sem, win_sem, out_sem, in_sem, ret_sem, back_sem):
    size_b, size_x, cap = dims
    n = size_x
    rows = ids_ref.shape[0]
    num_experts = 2 * size_b * size_x
    tok_dev, chunk = tok_hbm.shape[0], stage.shape[1]
    i_dp, i_b, i_a = lax.axis_index("dp"), lax.axis_index("ep_b"), lax.axis_index("ep_a")
    pos_x, core, pos_y = i_a // 2, lax.rem(i_a, 2), i_b
    pos = (1 - core) * pos_x + core * pos_y
    wpos = (1 - core) * pos_y + core * pos_x

    def sends_to(kind, k):
        return i_dp, (1 - kind) * pos_y + kind * k, 2 * ((1 - kind) * k + kind * pos_x) + kind

    def serves(k, c):
        return i_dp, core * k + (1 - core) * pos_y, 2 * (core * pos_x + (1 - core) * k) + c

    def shares(k):
        return i_dp, (1 - core) * k + core * pos_y, 2 * ((1 - core) * pos_x + core * k) + core

    def block(i):
        return pl.ds(pl.multiple_of(i * cap, cap), cap)

    def fetch(q):
        return pltpu.make_async_copy(tok_hbm.at[pl.ds(pl.multiple_of(q * chunk, chunk), chunk)], stage.at[lax.rem(q, 2)],
                                     tok_sem.at[lax.rem(q, 2)])

    def each_chunk(body):
        chunks = tok_dev // chunk

        def step(q, _):
            @pl.when(q + 1 < chunks)
            def _():
                fetch(q + 1).start()
            fetch(q).wait()
            body(q, lax.rem(q, 2))
            return 0

        lax.fori_loop(0, chunks, step, 0)

    fetch(0).start()
    held = ((w1_hbm, w1), (w2_hbm, w2), (b1_hbm, b1), (b2_hbm, b2))
    arrived = {1: (w1_next, w2_next), n - 1: (w1_last, w2_last)}
    for i, (own, every) in enumerate(held):
        pltpu.make_async_copy(own, every.at[pl.ds(0, 1)], win_sem.at[i, 0]).start()
    for d, pair in arrived.items():
        for i, matrix in enumerate(pair):
            pltpu.make_async_copy(matrix, held[i][1].at[pl.ds(d, 1)], win_sem.at[i, d]).start()

    barrier = pltpu.get_barrier_semaphore()
    for k in range(n):
        for c in range(2):
            for device in (sends_to(c, k), serves(k, c)):
                pl.semaphore_signal(barrier, inc=1, device_id=device, device_id_type=MESH_ID)
    for d in range(1, n):
        pl.semaphore_signal(barrier, inc=1, device_id=shares(lax.rem(wpos + d, n)), device_id_type=MESH_ID)
    pl.semaphore_wait(barrier, 5 * n - 1)

    def weight_copy(i, d):
        own, every = held[i]
        return pltpu.make_async_remote_copy(
            src_ref=own, dst_ref=every.at[pl.ds(d, 1)], send_sem=wout_sem.at[i, d], recv_sem=win_sem.at[i, d],
            device_id=shares(lax.rem(wpos - d + n, n)), device_id_type=MESH_ID)

    near, far = [1, n - 1], list(range(2, n - 1))
    for d in near + far:
        for i in (2, 3):
            weight_copy(i, d).start()

    def passed_on(i):
        every = held[i][1]
        to = (wpos - 1 + n, wpos + 1)[i]
        return pltpu.make_async_remote_copy(
            src_ref=arrived[near[i]][i], dst_ref=every.at[pl.ds(2, 1)], send_sem=wout_sem.at[i, 2], recv_sem=win_sem.at[i, 2],
            device_id=shares(lax.rem(to, n)), device_id_type=MESH_ID)

    def weights_here(i, off):
        own, every = held[i]
        pltpu.make_async_copy(own, every.at[pl.ds(off, 1)], win_sem.at[i, off]).wait()

    iota_exp = iota((num_experts, LANES), 0)

    soon = [0] + near
    send_order = [(step, off, kind) for offs, group in ((soon, near), (soon, far), (soon, [0]), (far, near + far + [0]))
                  for off in offs for step in group for kind in range(2)]

    def outgoing(t):
        step, off, kind = (pick([e[i] for e in send_order], t) for i in range(3))
        k = lax.rem((1 - kind) * pos_x + kind * pos_y + step, n)
        j = lax.rem((1 - kind) * pos_y + kind * pos_x + off, n)
        return step, kind, k, j

    def send_block(t):
        step, kind, k, j = outgoing(t)
        src = (kind * n + k) * n + j
        dst = (((1 - kind) * pos_x + kind * pos_y) * n + j) * 2 + core
        own = (step == 0) & (kind == core)

        @pl.when(own)
        def _():
            pltpu.make_async_copy(send.at[block(src)], recv.at[block(dst)], in_sem.at[dst]).start()

        @pl.when(jnp.logical_not(own))
        def _():
            pltpu.make_async_remote_copy(
                src_ref=send.at[block(src)], dst_ref=recv.at[block(dst)], send_sem=out_sem.at[src], recv_sem=in_sem.at[dst],
                device_id=sends_to(kind, k), device_id_type=MESH_ID).start()

    blocks = 2 * n * n
    early = 2 * len(soon) * len(near)
    lax.fori_loop(0, early, lambda t, _: (send_block(t), 0)[1], 0)
    for i in range(2):
        passed_on(i).start()
    lax.fori_loop(early, blocks, lambda t, _: (send_block(t), 0)[1], 0)

    keys = keys_ref[...].astype(F32)
    key_unit = keys / jnp.sqrt(jnp.sum(keys * keys, axis=1, keepdims=True))
    tau = tau_ref[0, 0]
    key_pad = jnp.concatenate([key_unit, jnp.zeros((LANES - num_experts, key_unit.shape[1]), F32)], axis=0)
    span = chunk // LANES

    def gate_rows(i, slot):
        r = jnp.dot(stage[slot], wr_ref[...], preferred_element_type=F32)
        unit = r / jnp.sqrt(jnp.sum(r * r, axis=1, keepdims=True))
        dots = lax.dot_general(unit, key_pad, (((1,), (1,)), ((), ())), preferred_element_type=F32,
                               precision=lax.Precision.HIGHEST)
        logits = dots.T[:num_experts] / tau
        p = jnp.exp(logits - jnp.max(logits, axis=0, keepdims=True))
        total = jnp.sum(p, axis=0, keepdims=True)
        for q in range(span):
            mine = iota_exp == ids_ref[pl.ds(i * span + q, 1), :]
            cols = slice(q * LANES, (q + 1) * LANES)
            gate_ref[pl.ds(i * span + q, 1), :] = jnp.sum(jnp.where(mine, p[:, cols], 0.0), axis=0, keepdims=True) / total[:, cols]

    each_chunk(gate_rows)

    serve_order = ([(0, off) for off in soon] + [(step, off) for off in soon for step in near]
                   + [(step, off) for step in far for off in soon] + [(step, off) for off in far for step in near + far + [0]])
    first_use = [[int(off not in [o for _, o in serve_order[:t]])
                  for t, (_, off) in enumerate(serve_order)] for i in range(len(held))]

    def incoming(t):
        step, off = (pick([e[i] for e in serve_order], t) for i in range(2))
        return lax.rem(pos - step + n, n), off, lax.rem(wpos + off, n)

    def result_ends(t, c):
        k, _, j = incoming(t)
        src, dst = (k * n + j) * 2 + c, (core * n + pos) * n + j
        return k, src, dst, (k == pos) & (core == c)

    def send_results(t):
        for c in range(2):
            k, src, dst, own = result_ends(t, c)

            @pl.when(own)
            def _():
                pltpu.make_async_copy(recv.at[block(src)], back_hbm.at[block(dst)], back_sem.at[dst]).start()

            @pl.when(jnp.logical_not(own))
            def _():
                pltpu.make_async_remote_copy(
                    src_ref=recv.at[block(src)], dst_ref=back_hbm.at[block(dst)], send_sem=ret_sem.at[src],
                    recv_sem=back_sem.at[dst], device_id=serves(k, c), device_id_type=MESH_ID).start()

    def serve(t, _):
        k, off, j = incoming(t)
        first = (k * n + j) * 2

        for i in range(len(held)):
            @pl.when(pick(first_use[i], t) == 1)
            def _():
                weights_here(i, off)

        for c in range(2):
            pltpu.make_async_copy(send.at[block(0)], recv.at[block(first + c)], in_sem.at[first + c]).wait()
        here = pl.ds(pl.multiple_of(first * cap, 2 * cap), 2 * cap)
        hidden = jnp.dot(recv[here, :], w1[off], preferred_element_type=F32) + b1[off].astype(F32)
        hidden = (0.5 * hidden * (1.0 + lax.erf(hidden * (0.5 ** 0.5)))).astype(BF16)
        y = jnp.dot(hidden, w2[off], preferred_element_type=F32) + b2[off].astype(F32)
        recv[here, :] = y.astype(BF16)

        @pl.when(t > 0)
        def _():
            send_results(t - 1)
        return 0

    lax.fori_loop(0, n * n, serve, 0)
    send_results(jnp.int32(n * n - 1))

    for i in range(2):
        passed_on(i).wait_send()
        for d in near + far:
            weight_copy(2 + i, d).wait_send()

    def drain(t, _):
        sent = pltpu.make_async_remote_copy(
            src_ref=send.at[block(t)], dst_ref=recv.at[block(t)], send_sem=out_sem.at[t], recv_sem=in_sem.at[t],
            device_id=(i_dp, i_b, i_a), device_id_type=MESH_ID)
        returned = pltpu.make_async_remote_copy(
            src_ref=recv.at[block(t)], dst_ref=back_hbm.at[block(t)], send_sem=ret_sem.at[t], recv_sem=back_sem.at[t],
            device_id=(i_dp, i_b, i_a), device_id_type=MESH_ID)
        kind, k = t // (n * n), lax.rem(t // n, n)

        @pl.when((kind != core) | (k != pos))
        def _():
            sent.wait_send()

        @pl.when((t // (2 * n) != pos) | (lax.rem(t, 2) != core))
        def _():
            returned.wait_send()

        returned.wait_recv()
        return 0

    lax.fori_loop(0, blocks, drain, 0)


def experts(tok_rows, ids, send_rows, w_route, expert_keys, temperature, weights, b1, b2, dims):
    size_b, size_x, cap = dims
    n = size_x
    tok_dev, width = tok_rows.shape
    hidden = weights[0].shape[2]
    slots = send_rows.shape[0]
    vmem, smem, hbm = (pl.BlockSpec(memory_space=m) for m in (pltpu.VMEM, pltpu.SMEM, pltpu.HBM))
    dma = pltpu.SemaphoreType.DMA
    return pl.pallas_call(
        functools.partial(experts_kernel, dims),
        name="experts",
        out_shape=(jax.ShapeDtypeStruct((slots, width), BF16), jax.ShapeDtypeStruct(ids.shape, F32)),
        in_specs=[vmem] * 3 + [smem] + [hbm] * (4 + len(weights)),
        out_specs=(hbm, vmem),
        scratch_shapes=[
            pltpu.VMEM((2, min(tok_dev, 512), width), BF16),
            pltpu.VMEM((slots, width), BF16),
            pltpu.VMEM((n, width, hidden), BF16),
            pltpu.VMEM((n, hidden, width), BF16),
            pltpu.VMEM((n, 1, hidden), BF16),
            pltpu.VMEM((n, 1, width), BF16),
            dma((2,)), dma((4, n)), dma((4, n)),
            dma((2 * n * n,)), dma((2 * n * n,)), dma((2 * n * n,)), dma((2 * n * n,)),
        ],
        compiler_params=pltpu.CompilerParams(collective_id=1, has_side_effects=True, vmem_limit_bytes=61 << 20),
        cost_estimate=pl.CostEstimate(flops=4 * slots * width * hidden, bytes_accessed=30_000_000, transcendentals=0),
    )(ids, w_route, expert_keys, temperature.reshape(1, 1), tok_rows, send_rows, *weights, b1, b2)


def combine_kernel(back_hbm, dest_hbm, gate_hbm, out_ref, stage, big, tmp, dest_even, dest_odd, gate_ref, sem, table_sem, gate_sem):
    i = pl.program_id(0)
    table_rows = dest_even.shape[0]

    def fetch_table(q, table, parity):
        return pltpu.make_async_copy(dest_hbm.at[pl.ds(pl.multiple_of(q * table_rows, table_rows), table_rows)], table,
                                     table_sem.at[parity])

    slots, width = back_hbm.shape
    parts = width // LANES
    chunk = stage.shape[1]
    chunks = slots // chunk

    @pl.when(i == 0)
    def _():
        def fetch(q):
            return pltpu.make_async_copy(back_hbm.at[pl.ds(pl.multiple_of(q * chunk, chunk), chunk)], stage.at[q], sem.at[q])

        for q in range(chunks):
            fetch(q).start()
        fetch_table(0, dest_even, 0).start()
        gate_copy = pltpu.make_async_copy(gate_hbm, gate_ref, gate_sem)
        gate_copy.start()
        big[pl.ds(slots * parts, 8), :] = jnp.zeros((8, LANES), F32)

        def widen_chunk(q, _):
            fetch(q).wait()

            def widen(u, _):
                base = pl.multiple_of(u * 16, 16)
                for c in range(parts):
                    big[pl.ds((q * chunk + base) * parts + c, 16, stride=parts), :] = (
                        stage[q, pl.ds(base, 16), c * LANES:(c + 1) * LANES].astype(F32))
                return 0

            lax.fori_loop(0, chunk // 16, widen, 0, unroll=8)
            return 0

        lax.fori_loop(0, chunks, widen_chunk, 0)
        gate_copy.wait()

    tables = (dest_even, dest_odd)
    for parity in range(2):
        @pl.when(lax.rem(i, 2) == parity)
        def _():
            table = tables[parity]

            @pl.when(i + 1 < pl.num_programs(0))
            def _():
                fetch_table(i + 1, tables[1 - parity], 1 - parity).start()
            fetch_table(i, table, parity).wait()

            for g in range(table_rows):
                base = g % 2 * (tmp.shape[0] // 2)
                for j in range(LANES):
                    tmp[pl.ds(base + j * parts, parts), :] = big[pl.ds(table[g, j], parts), :]
                gate = jnp.broadcast_to(gate_ref[pl.ds(i * table_rows + g, 1), :], (LANES, LANES)).T
                for j in range(0, LANES, 16):
                    for c in range(parts):
                        out_ref[g * LANES + j:g * LANES + j + 16, c * LANES:(c + 1) * LANES] = (
                            (gate[j:j + 16] * tmp[pl.ds(base + j * parts + c, 16, stride=parts), :]).astype(BF16))


def combine(back_rows, dest, gate, tok_dev):
    slots, width = back_rows.shape
    parts = width // LANES
    block = 1024
    hbm = pl.BlockSpec(memory_space=pltpu.HBM)
    return pl.pallas_call(
        combine_kernel,
        name="combine",
        grid=(tok_dev // block,),
        out_shape=jax.ShapeDtypeStruct((tok_dev, width), BF16),
        in_specs=[hbm] * 3,
        out_specs=pl.BlockSpec((block, width), lambda i: (i, 0)),
        scratch_shapes=[
            pltpu.VMEM((8, slots // 8, width), BF16),
            pltpu.VMEM((slots * parts + 8, LANES), F32),
            pltpu.VMEM((2 * (LANES * parts + 8), LANES), F32),
            pltpu.SMEM((block // LANES, LANES), jnp.int32),
            pltpu.SMEM((block // LANES, LANES), jnp.int32),
            pltpu.VMEM(gate.shape, F32),
            pltpu.SemaphoreType.DMA((8,)),
            pltpu.SemaphoreType.DMA((2,)),
            pltpu.SemaphoreType.DMA,
        ],
        compiler_params=pltpu.CompilerParams(vmem_limit_bytes=61 << 20, dimension_semantics=("arbitrary",)),
        cost_estimate=pl.CostEstimate(flops=20_000_000_000, bytes_accessed=15_000_000, transcendentals=0),
    )(back_rows, dest, gate)


def solution(mesh):
    size_b, size_x = mesh.shape["ep_b"], mesh.shape["ep_a"] // 2
    num_experts = 2 * size_b * size_x
    tok_spec = P(("dp",) + EXPERT_AXES)
    expert_spec = P(EXPERT_AXES)

    def from_place(d, w):
        pairs = []
        for y in range(size_b):
            for x in range(size_x):
                pairs.append(((y * size_x + x) * 2, (((y - d) % size_b) * size_x + x) * 2))
                pairs.append(((y * size_x + x) * 2 + 1, (y * size_x + (x - d) % size_x) * 2 + 1))
        return lax.ppermute(w, EXPERT_AXES, pairs)

    def device_step(tokens, expert_ids, route_order, w_route, expert_keys, temperature, w_in, b_in, w_out, b_out):
        tok_dev = tokens.shape[1]
        cap = (5 * tok_dev + 4 * num_experts - 1) // (4 * num_experts)
        dims = (size_b, size_x, cap)
        ids = expert_ids.reshape(tok_dev // LANES, LANES)
        weights = [w_in, w_out] + [from_place(d, w) for d in (1, size_x - 1) for w in (w_in, w_out)]
        send_rows, dest = dispatch(tokens[0], ids, route_order.reshape(ids.shape), dims)
        back_rows, gate = experts(tokens[0], ids, send_rows, w_route, expert_keys, temperature, weights,
                                  b_in[:, None, :], b_out[:, None, :], dims)
        return combine(back_rows, dest, gate, tok_dev)[None]

    return jax.shard_map(
        device_step,
        mesh=mesh,
        in_specs=(tok_spec, tok_spec, tok_spec, P(), P(), P(), expert_spec, expert_spec, expert_spec, expert_spec),
        out_specs=tok_spec,
        check_vma=False,
    )
```
